128 devices in a mesh: rows: 16 (over x, z), cols: 8 (over y, core).
Axes of the slice: x: 4, y: 4, z: 4, core: 2. Of those that a mesh axis runs over, the one named last changes fastest.
Arguments:
- bag_index: int32 [2048, 128], P(('rows', 'cols')), may hold values from 0 to 1048575, as said below
- bag_length: int32 [2048, 4], P(('rows', 'cols')), may hold values from 1 to 32
- emb_tables: float32 [4, 1048576, 128], P(None, ('rows', 'cols')), may hold values from -0.6 to 0.6
- dense_feats: float32 [2048, 128], P(('rows', 'cols')), may hold values from -6 to 6
- w_dense: float32 [128, 1024], replicated, may hold values from -0.5 to 0.5
- w_pair: float32 [10, 1024], replicated, may hold values from -0.5 to 0.5
- top_bias: float32 [1024], replicated, may hold values from -3 to 3
Outputs:
- pooled: float32 [2048, 4, 128], P(('rows', 'cols'))
- top_hidden: float32 [2048, 1024], P(('rows', 'cols'))
The draws below stay inside these ranges and needn't reach their ends.
Inputs may be any that keep to these rules, and one draw needn't show every extreme that they name: `bag_length`: slots at or past a bag's length are ignored, whatever they hold. `bag_index`: device d holds rows d * 8192 to (d + 1) * 8192 - 1 of every table; among the 2048 slots (live or not) of the samples of one device, at most 32 hold rows of any one device, and in every draw some device's rows receive exactly 32 slots from every device.
All inputs are finite; a program needn't handle non-finite values.
Results may differ from the reference program's by a relative error of at most 0.0001.
Values sent between devices are 32-bit elements; how exact they have to be, the bound alone decides.
A program may use at most 128 MiB of HBM per device.

```python
import jax
import jax.numpy as jnp
from jax import lax

E = 128
ROWS_DEV = 8192
NT = 4
L = 32
H = 1024
SAMP_DEV = 16
B = 2048
VOCAB = 1048576
PAIRS = 10


def draw_bag_index(key, part):
    ndevices = B // SAMP_DEV
    slots = SAMP_DEV * NT * L
    capacity = 2 * slots // ndevices
    total = ndevices * capacity
    token_owner = jnp.arange(total, dtype=jnp.int32) // capacity
    key_weight, key_common, key_blocks = jax.random.split(key, 3)
    weight = jax.random.randint(key_weight, (ndevices,), 0, 4, dtype=jnp.int32) * 512
    common_hot = jax.random.randint(key_common, (), 0, ndevices, dtype=jnp.int32)

    def one_block(block_key):
        key_own, key_score, key_order, key_first, key_second = jax.random.split(block_key, 5)
        own_hot = jax.random.randint(key_own, (), 0, ndevices, dtype=jnp.int32)
        forced = jnp.where((token_owner == common_hot) | (token_owner == own_hot), 4096, 0).astype(jnp.int32)
        score = jax.random.randint(key_score, (total,), 0, 1024, dtype=jnp.int32) + weight[token_owner] + forced
        score = score * total + jnp.arange(total, dtype=jnp.int32)
        unused, chosen = lax.top_k(score, slots)
        order = jax.random.permutation(key_order, slots)
        owners = token_owner[chosen[order]]
        first_draw = jax.random.randint(key_first, (slots,), 0, ROWS_DEV, dtype=jnp.int32)
        second_draw = jax.random.randint(key_second, (slots,), 1, ROWS_DEV + 1, dtype=jnp.int32)
        local = first_draw * second_draw // ROWS_DEV
        return (owners * ROWS_DEV + local).reshape(SAMP_DEV, NT * L)
    block_keys = jax.random.split(key_blocks, ndevices)
    return jax.vmap(one_block)(block_keys).reshape(B, NT * L).astype(jnp.int32)


def touch_ends(drawn, own_key, least, largest):
    dims = drawn.shape
    spot = [jax.random.randint(jax.random.fold_in(own_key, axis), (), 0, dims[axis]) for axis in range(len(dims))]
    drawn = drawn.at[tuple(spot)].set(least)
    longest = dims.index(max(dims))
    spot[longest] = (spot[longest] + 1) % dims[longest]
    return drawn.at[tuple(spot)].set(largest)


def block_scale(own_key, extent, cuts, smallest, largest):
    factor_of = 1.0
    for axis_at, parts in cuts:
        draws = jax.random.uniform(jax.random.fold_in(jax.random.fold_in(own_key, 6), axis_at), (parts,), jnp.float32, smallest / len(cuts), largest / len(cuts))
        factor_of = factor_of * jnp.repeat(jnp.exp(draws), extent[axis_at] // parts).reshape((-1,) + (1,) * (len(extent) - 1 - axis_at))
    return factor_of


def normal_values(stream_key, shape, spread, bound, cuts=(), held_as=jnp.bfloat16):
    drawn = spread * jax.random.normal(stream_key, shape, jnp.float32)
    if cuts:
        drawn = drawn * block_scale(stream_key, shape, cuts, -0.22, 0.18)
    return jnp.clip(drawn, -bound, bound).astype(held_as)


def setup_inputs(seed: int = 0) -> dict:
    seeds = jax.random.split(jax.random.key(seed), 8)
    return {
        "bag_index": draw_bag_index(jax.random.fold_in(seeds[7], 71), 0),
        "bag_length": touch_ends(jax.random.randint(seeds[1], (B, NT), 1, L + 1), jax.random.fold_in(seeds[1], 1), 1, L).astype(jnp.int32),
        "emb_tables": normal_values(seeds[2], (NT, VOCAB, E), 0.1, 0.6, ((1, 128),), jnp.float32),
        "dense_feats": normal_values(seeds[3], (B, E), 1.0, 6.0, ((0, 128),), jnp.float32),
        "w_dense": normal_values(seeds[4], (E, H), (E + PAIRS) ** -0.5, 0.5, (), jnp.float32),
        "w_pair": normal_values(seeds[5], (PAIRS, H), (E + PAIRS) ** -0.5, 0.5, (), jnp.float32),
        "top_bias": normal_values(seeds[6], (H,), 0.5, 3.0, (), jnp.float32),
    }


def interact(dense_feats, pooled, w_dense, w_pair, top_bias):
    feats = [dense_feats] + [pooled[:, t, :] for t in range(NT)]
    pair_list = []
    for first in range(NT + 1):
        for second in range(first + 1, NT + 1):
            pair_list.append(jnp.sum(feats[first] * feats[second], axis=-1))
    pair_dots = jnp.stack(pair_list, axis=1)
    hidden = jnp.dot(dense_feats, w_dense, precision=lax.Precision.HIGHEST, preferred_element_type=jnp.float32)
    hidden = hidden + jnp.dot(pair_dots, w_pair, precision=lax.Precision.HIGHEST, preferred_element_type=jnp.float32)
    return jnp.maximum(hidden + top_bias, 0.0)


def reference(bag_index, bag_length, emb_tables, dense_feats, w_dense, w_pair, top_bias):
    position = jnp.arange(L, dtype=jnp.int32)
    pieces = []
    for table in range(NT):
        ids = bag_index[:, table * L:(table + 1) * L]
        live = position[None, :] < bag_length[:, table:table + 1]
        picked = jnp.take(emb_tables[table], ids, axis=0)
        pieces.append(jnp.sum(jnp.where(live[:, :, None], picked, 0.0), axis=1))
    pooled = jnp.stack(pieces, axis=1)
    return pooled, interact(dense_feats, pooled, w_dense, w_pair, top_bias)
```

```python
import functools

import jax
import jax.numpy as jnp
from jax import lax
from jax.experimental import pallas as pl
from jax.experimental.pallas import tpu as pltpu
from jax.sharding import PartitionSpec as P

NT = 4
L = 32
E = 128
NDEV = 128
CAP = 32
BAGS = 64
MIX, UNMIX = 37, 45
CHUNKS = 4
TAB_PARTS = 8
MESH = pl.DeviceIdType.MESH
F32, BF16, I32 = jnp.float32, jnp.bfloat16, jnp.int32
NT_DIMS = (((1,), (1,)), ((), ()))
TN_DIMS = (((0,), (0,)), ((), ()))
NN_DIMS = (((1,), (0,)), ((), ()))


def dot(a, b, dims=NN_DIMS):
    return lax.dot_general(a, b, dims, preferred_element_type=F32)


def split2(v):
    hi = v.astype(BF16)
    return hi, (v - hi.astype(F32)).astype(BF16)


def position():
    r, c = lax.axis_index("rows"), lax.axis_index("cols")
    return lax.div(r, 4), lax.rem(r, 4), lax.div(c, 2), lax.rem(c, 2)


def shifted(me, step, sign):
    s = lax.rem(step * MIX, NDEV)
    digits = (lax.div(s, 32), lax.rem(lax.div(s, 8), 4), lax.rem(lax.div(s, 2), 4), lax.rem(s, 2))
    sizes = (4, 4, 4, 2)
    x, z, y, c = [lax.rem(m + n + sign * d, n) for m, d, n in zip(me, digits, sizes)]
    return x * 4 + z, y * 2 + c


def kernel(idx_hbm, len_hbm, tab_hbm, dense_hbm, wd_hbm, wp_hbm, bias_hbm, pooled_out, hidden_out,
           idx_ref, len_ref, tab, dense_ref, wd, wp, bias, ohs, vhi, vlo, vbag, outbox, inbox, checked, ids, gath, fetched, wsel,
           load_sem, tab_sem, ids_send, ids_recv, smem_sem, row_send, row_recv):
    me = position()
    loads = [pltpu.make_async_copy(s, d, load_sem.at[n]) for n, (s, d) in
             enumerate(((idx_hbm, idx_ref), (len_hbm, len_ref), (dense_hbm, dense_ref), (wd_hbm, wd), (wp_hbm, wp),
                        (bias_hbm, bias)))]
    part = tab.shape[0] // TAB_PARTS
    tab_loads = [pltpu.make_async_copy(tab_hbm.at[pl.ds(n * part, part)], tab.at[pl.ds(n * part, part)], tab_sem.at[n])
                 for n in range(TAB_PARTS)]

    for cp in loads[:2] + tab_loads + loads[2:]:
        cp.start()
    barrier = pltpu.get_barrier_semaphore()

    @pl.loop(1, NDEV)
    def _(step):
        pl.semaphore_signal(barrier, inc=1, device_id=shifted(me, step, 1), device_id_type=MESH)


    for cp in loads[:2]:
        cp.wait()
    idx = idx_ref[...]
    local_rows = tab.shape[0] // NT
    lane = lax.broadcasted_iota(I32, (16, NDEV), 1)
    table_of = lane // L
    of_table = (lax.broadcasted_iota(I32, (NT, NDEV), 1) // L == lax.broadcasted_iota(I32, (NT, NDEV), 0)).astype(F32)
    limit = dot(len_ref[...].astype(F32), of_table, TN_DIMS).astype(I32)
    live = lane % L < limit
    owner = idx // local_rows
    code = table_of * local_rows + idx % local_rows
    ox, oz, oy, oc = owner // 32, owner // 8 % 4, owner // 2 % 4, owner % 2
    x, z, y, c = me
    s = (ox - x + 4) % 4 * 32 + (oz - z + 4) % 4 * 8 + (oy - y + 4) % 4 * 2 + (oc - c + 2) % 2
    rel = jnp.where(live, s * UNMIX % NDEV, -1)
    bag = lax.broadcasted_iota(I32, (16, NDEV), 0) + 16 * table_of + 1
    sub = lax.broadcasted_iota(I32, (NDEV, NDEV), 0)
    lan = lax.broadcasted_iota(I32, (NDEV, NDEV), 1)
    before = jnp.concatenate([(sub < lan).astype(F32), jnp.ones((NDEV, NDEV), F32)], axis=1).astype(BF16)
    code_hi, code_lo, bag = (code // 256).astype(F32), (code % 256).astype(F32), bag.astype(F32)
    carry = jnp.zeros((NDEV, NDEV), F32)
    for r in range(16):
        oh = (sub == rel[r:r + 1, :]).astype(F32)
        ohb = oh.astype(BF16)
        counts = dot(ohb, before)
        rank = jnp.sum(oh * (counts[:, :NDEV] + carry), axis=0, keepdims=True).astype(I32)
        carry = carry + counts[:, NDEV:]
        cols = slice(r * NDEV, (r + 1) * NDEV)
        here = sub[:CAP] == rank
        ohs[:, cols] = ohb
        vhi[:, cols] = jnp.where(here, code_hi[r:r + 1], 0.0).astype(BF16)
        vlo[:, cols] = jnp.where(here, code_lo[r:r + 1], 0.0).astype(BF16)
        vbag[:, cols] = jnp.where(sub % CAP == rank, bag[r:r + 1], 0.0).astype(BF16)
    all_oh = ohs[...]
    box = dot(all_oh, vhi[...], NT_DIMS) * 256.0 + dot(all_oh, vlo[...], NT_DIMS)
    outbox[...] = box.astype(I32).reshape(NDEV, 1, CAP)
    inbox[0] = outbox[0]

    pl.semaphore_wait(barrier, NDEV - 1)

    def ids_copy(step):
        return pltpu.make_async_remote_copy(
            src_ref=outbox.at[step], dst_ref=inbox.at[step], send_sem=ids_send, recv_sem=ids_recv,
            device_id=shifted(me, step, 1), device_id_type=MESH)

    @pl.loop(1, NDEV)
    def _(step):
        ids_copy(step).start()

    bags = dot(all_oh, vbag[...], NT_DIMS)
    bags = jnp.where(lan // CAP == sub % 4, bags, 0.0).astype(BF16)
    groups = NDEV // 4
    gather4 = (lax.broadcasted_iota(I32, (groups, NDEV), 1) // 4
               == lax.broadcasted_iota(I32, (groups, NDEV), 0)).astype(F32).astype(BF16)
    group_bags = dot(gather4, bags).astype(I32)
    want = lax.broadcasted_iota(I32, (BAGS, NDEV), 0) + 1
    for g in range(groups):
        wsel[:, g * NDEV:(g + 1) * NDEV] = (want == group_bags[g:g + 1, :]).astype(F32).astype(BF16)
    for cp in loads[2:]:
        cp.wait()
    dense = dense_ref[...]
    hidden = lax.dot_general(dense, wd[...], NN_DIMS, precision=lax.Precision.HIGHEST,
                             preferred_element_type=F32) + bias[...]
    for cp in tab_loads:
        cp.wait()

    whole = pltpu.make_async_remote_copy(
        src_ref=outbox.at[pl.ds(1, NDEV - 1)], dst_ref=inbox.at[pl.ds(1, NDEV - 1)], send_sem=ids_send,
        recv_sem=ids_recv, device_id=shifted(me, 1, 1), device_id_type=MESH)
    whole.wait_recv()
    checked[...] = jnp.clip(inbox[...], 0, tab.shape[0] - 1)
    to_smem = pltpu.make_async_copy(checked, ids, smem_sem)
    to_smem.start()
    to_smem.wait()

    per = NDEV // CHUNKS

    def gather(step, dst):
        for j in range(CAP):
            dst[step, j:j + 1, :] = tab[pl.ds(ids[step, 0, j], 1), :]

    def row_copy(step, chunk):
        return pltpu.make_async_remote_copy(
            src_ref=gath.at[step], dst_ref=fetched.at[step], send_sem=row_send.at[0], recv_sem=row_recv.at[chunk],
            device_id=shifted(me, step, -1), device_id_type=MESH)

    gather(0, fetched)
    for chunk in range(CHUNKS):
        @pl.loop(1 if chunk == 0 else chunk * per, (chunk + 1) * per)
        def _(step):
            gather(step, gath)
            row_copy(step, chunk).start()

    total = jnp.zeros((BAGS, E), F32)
    for chunk in range(CHUNKS):
        first = 1 if chunk == 0 else chunk * per
        span = pl.ds(first, (chunk + 1) * per - first)
        pltpu.make_async_remote_copy(
            src_ref=gath.at[span], dst_ref=fetched.at[span], send_sem=row_send.at[0], recv_sem=row_recv.at[chunk],
            device_id=shifted(me, 1, 1), device_id_type=MESH).wait_recv()
        got = fetched[chunk * per:(chunk + 1) * per].reshape(per * CAP, E)
        hi, lo = split2(got)
        w = wsel[:, chunk * per * CAP:(chunk + 1) * per * CAP]
        total = total + (dot(w, hi) + dot(w, lo))

    feats = [dense] + [total[t * 16:(t + 1) * 16] for t in range(NT)]
    for t in range(NT):
        pooled_out[:, t, :] = feats[t + 1]
    k = 0
    for a in range(NT + 1):
        for b in range(a + 1, NT + 1):
            d = jnp.sum(feats[a] * feats[b], axis=-1, keepdims=True)
            hidden = hidden + d * wp[k:k + 1, :]
            k += 1
    hidden_out[...] = jnp.maximum(hidden, 0.0)

    whole.wait_send()
    everything = pl.ds(1, NDEV - 1)
    pltpu.make_async_remote_copy(
        src_ref=gath.at[everything], dst_ref=fetched.at[everything], send_sem=row_send.at[0], recv_sem=row_recv.at[0],
        device_id=shifted(me, 1, 1), device_id_type=MESH).wait_send()


def shards(bag_index, bag_length, emb_tables, dense_feats, w_dense, w_pair, top_bias):
    rows = NT * emb_tables.shape[1]
    hidden = w_dense.shape[1]
    slots = 16 * NDEV
    vmem, hbm = pl.BlockSpec(memory_space=pltpu.VMEM), pl.BlockSpec(memory_space=pltpu.HBM)
    return pl.pallas_call(
        kernel,
        out_shape=(jax.ShapeDtypeStruct((16, NT, E), F32), jax.ShapeDtypeStruct((16, hidden), F32)),
        in_specs=[hbm] * 7,
        out_specs=(vmem, vmem),
        scratch_shapes=[
            pltpu.VMEM((16, NDEV), I32),
            pltpu.VMEM((NT, 16), I32),
            pltpu.VMEM((rows, E), F32),
            pltpu.VMEM((16, E), F32),
            pltpu.VMEM(w_dense.shape, F32),
            pltpu.VMEM(w_pair.shape, F32),
            pltpu.VMEM((1, hidden), F32),
            pltpu.VMEM((NDEV, slots), BF16),
            pltpu.VMEM((CAP, slots), BF16),
            pltpu.VMEM((CAP, slots), BF16),
            pltpu.VMEM((NDEV, slots), BF16),
            pltpu.VMEM((NDEV, 1, CAP), I32),
            pltpu.VMEM((NDEV, 1, CAP), I32),
            pltpu.VMEM((NDEV, 1, CAP), I32),
            pltpu.SMEM((NDEV, 1, CAP), I32),
            pltpu.VMEM((NDEV, CAP, E), F32),
            pltpu.VMEM((NDEV, CAP, E), F32),
            pltpu.VMEM((BAGS, NDEV * CAP), BF16),
            pltpu.SemaphoreType.DMA((6,)),
            pltpu.SemaphoreType.DMA((TAB_PARTS,)),
            pltpu.SemaphoreType.DMA,
            pltpu.SemaphoreType.DMA,
            pltpu.SemaphoreType.DMA,
            pltpu.SemaphoreType.DMA((1,)),
            pltpu.SemaphoreType.DMA((CHUNKS,)),
        ],
        compiler_params=pltpu.CompilerParams(
            collective_id=0, has_side_effects=True, vmem_limit_bytes=60 * 1024 * 1024),
    )(bag_index, bag_length.T, emb_tables.reshape(rows, E), dense_feats, w_dense, w_pair, top_bias.reshape(1, hidden))


def solution(mesh):
    samples = P(("rows", "cols"), None)
    in_specs = (samples, samples, P(None, ("rows", "cols"), None), samples, P(), P(), P())
    out_specs = (P(("rows", "cols"), None, None), samples)
    return jax.shard_map(shards, mesh=mesh, in_specs=in_specs, out_specs=out_specs, check_vma=False)
```

```python
import functools

import jax
import jax.numpy as jnp
from jax import lax
from jax.experimental import pallas as pl
from jax.experimental.pallas import tpu as pltpu
from jax.sharding import PartitionSpec as P

NT = 4
L = 32
E = 128
NDEV = 128
CAP = 32
BAGS = 64
TAB_PARTS = 8
MESH = pl.DeviceIdType.MESH
F32, BF16, I32 = jnp.float32, jnp.bfloat16, jnp.int32
NT_DIMS = (((1,), (1,)), ((), ()))
TN_DIMS = (((0,), (0,)), ((), ()))
NN_DIMS = (((1,), (0,)), ((), ()))


def dot(a, b, dims=NN_DIMS):
    return lax.dot_general(a, b, dims, preferred_element_type=F32)


def split2(v):
    hi = v.astype(BF16)
    return hi, (v - hi.astype(F32)).astype(BF16)


def position():
    r, c = lax.axis_index("rows"), lax.axis_index("cols")
    return lax.div(r, 4), lax.rem(r, 4), lax.div(c, 2), lax.rem(c, 2)


def around(at, n, sign=1):
    return [lax.rem(at + n + sign * d, n) for d in range(n)]


def kernel(idx_hbm, len_hbm, tab_hbm, dense_hbm, wd_hbm, wp_hbm, bias_hbm, pooled_out, hidden_out,
           idx_ref, len_ref, tab, dense_ref, wd, wp, bias, ohs, vhi, vlo, vbag, outbox, passing, inbox, checked, ids, mybags, linebags, stage, agg, sums, parts,
           load_sem, tab_sem, ids_send, ids_recv, smem_sem, bag_send, bag_recv, row_send, row_recv, sum_send, sum_recv):
    me = position()
    loads = [pltpu.make_async_copy(s, d, load_sem.at[n]) for n, (s, d) in
             enumerate(((idx_hbm, idx_ref), (len_hbm, len_ref), (dense_hbm, dense_ref), (wd_hbm, wd), (wp_hbm, wp),
                        (bias_hbm, bias)))]
    part = tab.shape[0] // TAB_PARTS
    tab_loads = [pltpu.make_async_copy(tab_hbm.at[pl.ds(n * part, part)], tab.at[pl.ds(n * part, part)], tab_sem.at[n])
                 for n in range(TAB_PARTS)]

    for cp in loads[:2] + tab_loads + loads[2:]:
        cp.start()
    barrier = pltpu.get_barrier_semaphore()

    my_row, my_col = lax.axis_index("rows"), lax.axis_index("cols")
    xs, zs, ys, cs = [around(at, n) for at, n in zip(me, (4, 4, 4, 2))]
    line = [(my_row, y * 2 + c) for y in ys for c in cs]
    plane = [(x * 4 + z, my_col) for x in xs for z in zs]
    for peer in plane[1:] + line[1:]:
        pl.semaphore_signal(barrier, inc=1, device_id=peer, device_id_type=MESH)


    for cp in loads[:2]:
        cp.wait()
    idx = idx_ref[...]
    local_rows = tab.shape[0] // NT
    lane = lax.broadcasted_iota(I32, (16, NDEV), 1)
    table_of = lane // L
    of_table = (lax.broadcasted_iota(I32, (NT, NDEV), 1) // L == lax.broadcasted_iota(I32, (NT, NDEV), 0)).astype(F32)
    limit = dot(len_ref[...].astype(F32), of_table, TN_DIMS).astype(I32)
    live = lane % L < limit
    owner = idx // local_rows
    code = table_of * local_rows + idx % local_rows
    ox, oz, oy, oc = owner // 32, owner // 8 % 4, owner // 2 % 4, owner % 2
    x, z, y, c = me
    slot = (oy - y + 4) % 4 * 32 + (oc - c + 2) % 2 * 16 + (ox - x + 4) % 4 * 4 + (oz - z + 4) % 4
    rel = jnp.where(live, slot, -1)
    bag = lax.broadcasted_iota(I32, (16, NDEV), 0) + 16 * table_of + 1
    sub = lax.broadcasted_iota(I32, (NDEV, NDEV), 0)
    lan = lax.broadcasted_iota(I32, (NDEV, NDEV), 1)
    before = jnp.concatenate([(sub < lan).astype(F32), jnp.ones((NDEV, NDEV), F32)], axis=1).astype(BF16)
    code_hi, code_lo, bag = (code // 256).astype(F32), (code % 256).astype(F32), bag.astype(F32)
    carry = jnp.zeros((NDEV, NDEV), F32)
    for r in range(16):
        oh = (sub == rel[r:r + 1, :]).astype(F32)
        ohb = oh.astype(BF16)
        counts = dot(ohb, before)
        rank = jnp.sum(oh * (counts[:, :NDEV] + carry), axis=0, keepdims=True).astype(I32)
        carry = carry + counts[:, NDEV:]
        cols = slice(r * NDEV, (r + 1) * NDEV)
        here = sub[:CAP] == rank
        ohs[:, cols] = ohb
        vhi[:, cols] = jnp.where(here, code_hi[r:r + 1], 0.0).astype(BF16)
        vlo[:, cols] = jnp.where(here, code_lo[r:r + 1], 0.0).astype(BF16)
        vbag[:, cols] = jnp.where(sub % CAP == rank, bag[r:r + 1], 0.0).astype(BF16)
    all_oh = ohs[...]
    box = dot(all_oh, vhi[...], NT_DIMS) * 256.0 + dot(all_oh, vlo[...], NT_DIMS)
    outbox[...] = box.astype(I32).reshape(8, 16, 1, CAP)

    pl.semaphore_wait(barrier, 22)

    def line_copy(n):
        return pltpu.make_async_remote_copy(
            src_ref=outbox.at[n], dst_ref=passing.at[:, n], send_sem=ids_send.at[0], recv_sem=ids_recv.at[0],
            device_id=line[n], device_id_type=MESH)

    def plane_copy(n):
        return pltpu.make_async_remote_copy(
            src_ref=passing.at[n], dst_ref=inbox.at[n], send_sem=ids_send.at[1], recv_sem=ids_recv.at[1],
            device_id=plane[n], device_id_type=MESH)

    for n in range(1, 8):
        line_copy(n).start()
    passing[:, 0] = outbox[0]

    first = pltpu.make_async_remote_copy(
        src_ref=outbox.at[pl.ds(1, 7)], dst_ref=outbox.at[pl.ds(1, 7)], send_sem=ids_send.at[0],
        recv_sem=ids_recv.at[0], device_id=line[1], device_id_type=MESH)
    second = pltpu.make_async_remote_copy(
        src_ref=passing.at[pl.ds(1, 15)], dst_ref=inbox.at[pl.ds(1, 15)], send_sem=ids_send.at[1],
        recv_sem=ids_recv.at[1], device_id=plane[1], device_id_type=MESH)
    first.wait_recv()
    for n in range(1, 16):
        plane_copy(n).start()
    inbox[0] = passing[0]

    def device(kind, da, db, dy, core, sign):
        dx, dz = da + kind * (db - da), db + kind * (da - db)
        return (lax.rem(x + 4 + sign * dx, 4) * 4 + lax.rem(z + 4 + sign * dz, 4), lax.rem(y + 4 + sign * dy, 4) * 2 + core)

    def line_at(t, n):
        return (0, n, t) if n < 3 else (t, 3, 0)

    def line_order(slot):
        dy, dc, dx, dz = slot // 32, slot // 16 % 2, slot // 4 % 4, slot % 4
        da, db = dx + c * (dz - dx), dz + c * (dx - dz)
        on_y = db == 3
        t, member = jnp.where(on_y, da, dy), jnp.where(on_y, dy, da)
        return (t * 4 + db) * 2 + member // 2, member % 2 * 2 + (c + dc) % 2

    bags = dot(all_oh, vbag[...], NT_DIMS)
    bags = jnp.where(lan // CAP == line_order(sub)[1], bags, 0.0).astype(BF16)
    pick = (line_order(lan[:32])[0] == sub[:32]).astype(F32).astype(BF16)
    mybags[...] = dot(pick, bags).astype(I32).reshape(32, 1, NDEV)
    for cp in loads[2:]:
        cp.wait()
    dense = dense_ref[...]
    hidden = lax.dot_general(dense, wd[...], NN_DIMS, precision=lax.Precision.HIGHEST,
                             preferred_element_type=F32) + bias[...]
    for cp in tab_loads:
        cp.wait()

    second.wait_recv()

    def bags_copy(t, n):
        return pltpu.make_async_remote_copy(
            src_ref=mybags.at[pl.ds((t * 4 + n) * 2, 2)], dst_ref=linebags.at[pl.ds((t * 4 + n) * 2, 2)],
            send_sem=bag_send, recv_sem=bag_recv, device_id=device(c, *line_at(t, n), c, 1), device_id_type=MESH)

    for t in range(4):
        for n in range(4):
            if t or n:
                bags_copy(t, n).start()
    linebags[0:2] = mybags[0:2]
    checked[...] = jnp.clip(inbox[...].reshape(NDEV, 1, CAP), 0, tab.shape[0] - 1)
    to_smem = pltpu.make_async_copy(checked, ids, smem_sem)
    to_smem.start()
    to_smem.wait()

    def block(dst, at, e):
        for j in range(CAP):
            dst[(*at, slice(j, j + 1))] = tab[pl.ds(ids[e, 0, j], 1), :]

    def entry(kind, other, da, db, dy):
        return (da * (4 - 3 * kind) + db * (1 + 3 * kind)) * 8 + dy * 2 + other

    def rows_copy(src, dst, t, peer):
        return pltpu.make_async_remote_copy(
            src_ref=src, dst_ref=dst, send_sem=row_send, recv_sem=row_recv.at[t], device_id=peer, device_id_type=MESH)

    @pl.loop(0, 4)
    def _(t):
        for other in range(2):
            kind = c + other * (1 - 2 * c)
            base = (other * 4 + t) * 4

            def gather(m, dst, at):
                for n in range(4):
                    da, db, dy = (m, n, t) if n < 3 else (t, 3, m)
                    block(dst, at(m, n), entry(kind, other, da, db, dy))

            def send(m):
                if m == 0:
                    rows_copy(stage.at[base], agg.at[t, :, 0, c], t, (my_row, y * 2 + kind)).start()
                    return
                rows_copy(stage.at[base + m, pl.ds(0, 3)], agg.at[t, pl.ds(0, 3), m, c], t,
                          device(kind, m, 0, 0, kind, -1)).start()
                rows_copy(stage.at[base + m, 3], agg.at[t, 3, m, c], t, device(kind, 0, 0, m, kind, -1)).start()

            if other == 0:
                gather(0, agg, lambda m, n: (t, n, m, c))

            @pl.loop(1 - other, 4)
            def _(m):
                gather(m, stage, lambda m, n: (base + m, n))
            for m in range(1 - other, 4):
                send(m)

    def count(blocks, sem):
        return pltpu.make_async_remote_copy(
            src_ref=stage.at[pl.ds(0, blocks)], dst_ref=stage.at[pl.ds(0, blocks)], send_sem=sem, recv_sem=sem,
            device_id=line[1], device_id_type=MESH)

    all_bags = pltpu.make_async_remote_copy(
        src_ref=mybags.at[pl.ds(2, 30)], dst_ref=linebags.at[pl.ds(2, 30)], send_sem=bag_send, recv_sem=bag_recv,
        device_id=line[1], device_id_type=MESH)
    all_bags.wait_recv()
    want = lax.broadcasted_iota(I32, (BAGS, NDEV), 0) + 1

    def sum_copy(t, n):
        return pltpu.make_async_remote_copy(
            src_ref=sums.at[t * 4 + n], dst_ref=parts.at[t * 4 + n], send_sem=sum_send, recv_sem=sum_recv.at[t],
            device_id=device(c, *line_at(t, n), c, -1), device_id_type=MESH)

    def sums_of(t):
        begin = 1 if t == 0 else t * 4
        span = pl.ds(begin, t * 4 + 4 - begin)
        return pltpu.make_async_remote_copy(
            src_ref=sums.at[span], dst_ref=parts.at[span], send_sem=sum_send, recv_sem=sum_recv.at[t],
            device_id=line[1], device_id_type=MESH)

    for t in range(4):
        count(7, row_recv.at[t]).wait_recv()
        for n in range(4):
            at = (t * 4 + n) * 2
            w = jnp.concatenate([(want == linebags[at + h]).astype(F32) for h in range(2)], axis=1).astype(BF16)
            hi, lo = split2(agg[t, n].reshape(8 * CAP, E))
            part = dot(w, hi) + dot(w, lo)
            if t or n:
                sums[t * 4 + n] = part
                sum_copy(t, n).start()
            else:
                parts[0] = part

    total = jnp.zeros((BAGS, E), F32)
    for t in range(4):
        sums_of(t).wait_recv()
        for n in range(4):
            total = total + parts[t * 4 + n]

    feats = [dense] + [total[t * 16:(t + 1) * 16] for t in range(NT)]
    for t in range(NT):
        pooled_out[:, t, :] = feats[t + 1]
    k = 0
    for a in range(NT + 1):
        for b in range(a + 1, NT + 1):
            d = jnp.sum(feats[a] * feats[b], axis=-1, keepdims=True)
            hidden = hidden + d * wp[k:k + 1, :]
            k += 1
    hidden_out[...] = jnp.maximum(hidden, 0.0)

    first.wait_send()
    second.wait_send()
    all_bags.wait_send()
    count(28, row_send).wait_send()
    pltpu.make_async_remote_copy(
        src_ref=sums.at[pl.ds(1, 15)], dst_ref=parts.at[pl.ds(1, 15)], send_sem=sum_send, recv_sem=sum_recv.at[0],
        device_id=line[1], device_id_type=MESH).wait_send()


def put_out(pooled, hidden, pooled_out, hidden_out, sems):
    copies = [pltpu.make_async_copy(pooled, pooled_out, sems.at[0]), pltpu.make_async_copy(hidden, hidden_out, sems.at[1])]
    for cp in copies:
        cp.start()
    for cp in copies:
        cp.wait()


def shards(bag_index, bag_length, emb_tables, dense_feats, w_dense, w_pair, top_bias):
    rows = NT * emb_tables.shape[1]
    hidden = w_dense.shape[1]
    slots = 16 * NDEV
    vmem, hbm = pl.BlockSpec(memory_space=pltpu.VMEM), pl.BlockSpec(memory_space=pltpu.HBM)
    outs = (jax.ShapeDtypeStruct((16, NT, E), F32), jax.ShapeDtypeStruct((16, hidden), F32))
    found = pl.pallas_call(
        kernel,
        out_shape=outs,
        in_specs=[hbm] * 7,
        out_specs=(vmem, vmem),
        scratch_shapes=[
            pltpu.VMEM((16, NDEV), I32),
            pltpu.VMEM((NT, 16), I32),
            pltpu.VMEM((rows, E), F32),
            pltpu.VMEM((16, E), F32),
            pltpu.VMEM(w_dense.shape, F32),
            pltpu.VMEM(w_pair.shape, F32),
            pltpu.VMEM((1, hidden), F32),
            pltpu.VMEM((NDEV, slots), BF16),
            pltpu.VMEM((CAP, slots), BF16),
            pltpu.VMEM((CAP, slots), BF16),
            pltpu.VMEM((NDEV, slots), BF16),
            pltpu.VMEM((8, 16, 1, CAP), I32),
            pltpu.VMEM((16, 8, 1, CAP), I32),
            pltpu.VMEM((16, 8, 1, CAP), I32),
            pltpu.VMEM((NDEV, 1, CAP), I32),
            pltpu.SMEM((NDEV, 1, CAP), I32),
            pltpu.VMEM((32, 1, NDEV), I32),
            pltpu.VMEM((32, 1, NDEV), I32),
            pltpu.VMEM((32, 4, CAP, E), F32),
            pltpu.VMEM((4, 4, 4, 2, CAP, E), F32),
            pltpu.VMEM((16, BAGS, E), F32),
            pltpu.VMEM((16, BAGS, E), F32),
            pltpu.SemaphoreType.DMA((6,)),
            pltpu.SemaphoreType.DMA((TAB_PARTS,)),
            pltpu.SemaphoreType.DMA((2,)),
            pltpu.SemaphoreType.DMA((2,)),
            pltpu.SemaphoreType.DMA,
            pltpu.SemaphoreType.DMA,
            pltpu.SemaphoreType.DMA,
            pltpu.SemaphoreType.DMA,
            pltpu.SemaphoreType.DMA((4,)),
            pltpu.SemaphoreType.DMA,
            pltpu.SemaphoreType.DMA((4,)),
        ],
        compiler_params=pltpu.CompilerParams(
            collective_id=0, has_side_effects=True, vmem_limit_bytes=60 * 1024 * 1024),
    )(bag_index, bag_length.T, emb_tables.reshape(rows, E), dense_feats, w_dense, w_pair, top_bias.reshape(1, hidden))
    return pl.pallas_call(
        put_out,
        out_shape=outs,
        in_specs=[vmem, vmem],
        out_specs=(hbm, hbm),
        compiler_params=pltpu.CompilerParams(vmem_limit_bytes=60 * 1024 * 1024),
        scratch_shapes=[pltpu.SemaphoreType.DMA((2,))],
    )(*found)


def solution(mesh):
    samples = P(("rows", "cols"), None)
    in_specs = (samples, samples, P(None, ("rows", "cols"), None), samples, P(), P(), P())
    out_specs = (P(("rows", "cols"), None, None), samples)
    return jax.shard_map(shards, mesh=mesh, in_specs=in_specs, out_specs=out_specs, check_vma=False)
```

```python
import functools

import jax
import jax.numpy as jnp
from jax import lax
from jax.experimental import pallas as pl
from jax.experimental.pallas import tpu as pltpu
from jax.sharding import PartitionSpec as P

NT = 4
L = 32
E = 128
NDEV = 128
CAP = 32
BAGS = 64
TAB_PARTS = 8
MESH = pl.DeviceIdType.MESH
F32, BF16, I32 = jnp.float32, jnp.bfloat16, jnp.int32
NT_DIMS = (((1,), (1,)), ((), ()))
TN_DIMS = (((0,), (0,)), ((), ()))
NN_DIMS = (((1,), (0,)), ((), ()))


def dot(a, b, dims=NN_DIMS):
    return lax.dot_general(a, b, dims, preferred_element_type=F32)


def split2(v):
    hi = v.astype(BF16)
    return hi, (v - hi.astype(F32)).astype(BF16)


def position():
    r, c = lax.axis_index("rows"), lax.axis_index("cols")
    return lax.div(r, 4), lax.rem(r, 4), lax.div(c, 2), lax.rem(c, 2)


def around(at, n, sign=1):
    return [lax.rem(at + n + sign * d, n) for d in range(n)]


def kernel(idx_hbm, len_hbm, tab_hbm, dense_hbm, wd_hbm, wp_hbm, bias_hbm, pooled_out, hidden_out,
           idx_ref, len_ref, tab, dense_ref, wd, wp, bias, ohs, vhi, vlo, vbag, outbox, passing, ids, mybags, linebags, stage, agg, sums, parts,
           load_sem, tab_sem, ids_send, ids_recv, smem_sem, bag_send, bag_recv, row_send, row_recv, sum_send, sum_recv):
    me = position()
    loads = [pltpu.make_async_copy(s, d, load_sem.at[n]) for n, (s, d) in
             enumerate(((idx_hbm, idx_ref), (len_hbm, len_ref), (dense_hbm, dense_ref), (wd_hbm, wd), (wp_hbm, wp),
                        (bias_hbm, bias)))]
    part = tab.shape[0] // TAB_PARTS
    tab_loads = [pltpu.make_async_copy(tab_hbm.at[pl.ds(n * part, part)], tab.at[pl.ds(n * part, part)], tab_sem.at[n])
                 for n in range(TAB_PARTS)]

    for cp in loads[:2] + tab_loads + loads[2:]:
        cp.start()
    barrier = pltpu.get_barrier_semaphore()

    my_row, my_col = lax.axis_index("rows"), lax.axis_index("cols")
    xs, zs, ys, cs = [around(at, n) for at, n in zip(me, (4, 4, 4, 2))]
    line = [(my_row, y * 2 + c) for y in ys for c in cs]
    plane = [(x * 4 + z, my_col) for x in xs for z in zs]
    for peer in plane[1:] + line[1:]:
        pl.semaphore_signal(barrier, inc=1, device_id=peer, device_id_type=MESH)


    for cp in loads[:2]:
        cp.wait()
    idx = idx_ref[...]
    local_rows = tab.shape[0] // NT
    lane = lax.broadcasted_iota(I32, (16, NDEV), 1)
    table_of = lane // L
    of_table = (lax.broadcasted_iota(I32, (NT, NDEV), 1) // L == lax.broadcasted_iota(I32, (NT, NDEV), 0)).astype(F32)
    limit = dot(len_ref[...].astype(F32), of_table, TN_DIMS).astype(I32)
    live = lane % L < limit
    owner = idx // local_rows
    code = table_of * local_rows + idx % local_rows
    ox, oz, oy, oc = owner // 32, owner // 8 % 4, owner // 2 % 4, owner % 2
    x, z, y, c = me
    slot = (oy - y + 4) % 4 * 32 + (oc - c + 2) % 2 * 16 + (ox - x + 4) % 4 * 4 + (oz - z + 4) % 4
    rel = jnp.where(live, slot, -1)
    bag = lax.broadcasted_iota(I32, (16, NDEV), 0) + 16 * table_of + 1
    sub = lax.broadcasted_iota(I32, (NDEV, NDEV), 0)
    lan = lax.broadcasted_iota(I32, (NDEV, NDEV), 1)
    before = jnp.concatenate([(sub < lan).astype(F32), jnp.ones((NDEV, NDEV), F32)], axis=1).astype(BF16)
    code_hi, code_lo, bag = (code // 256).astype(F32), (code % 256).astype(F32), bag.astype(F32)
    carry = jnp.zeros((NDEV, NDEV), F32)
    for r in range(16):
        oh = (sub == rel[r:r + 1, :]).astype(F32)
        ohb = oh.astype(BF16)
        counts = dot(ohb, before)
        rank = jnp.sum(oh * (counts[:, :NDEV] + carry), axis=0, keepdims=True).astype(I32)
        carry = carry + counts[:, NDEV:]
        cols = slice(r * NDEV, (r + 1) * NDEV)
        here = sub[:CAP] == rank
        ohs[:, cols] = ohb
        vhi[:, cols] = jnp.where(here, code_hi[r:r + 1], 0.0).astype(BF16)
        vlo[:, cols] = jnp.where(here, code_lo[r:r + 1], 0.0).astype(BF16)
        vbag[:, cols] = jnp.where(sub % CAP == rank, bag[r:r + 1], 0.0).astype(BF16)
    all_oh = ohs[...]
    box = dot(all_oh, vhi[...], NT_DIMS) * 256.0 + dot(all_oh, vlo[...], NT_DIMS)
    outbox[...] = jnp.clip(box.astype(I32), 0, tab.shape[0] - 1).reshape(8, 16, 1, CAP)

    pl.semaphore_wait(barrier, 22)

    def line_copy(n):
        return pltpu.make_async_remote_copy(
            src_ref=outbox.at[n], dst_ref=passing.at[:, n], send_sem=ids_send.at[0], recv_sem=ids_recv.at[0],
            device_id=line[n], device_id_type=MESH)

    def plane_copy(n):
        return pltpu.make_async_remote_copy(
            src_ref=passing.at[n], dst_ref=ids.at[pl.ds(n * 8, 8)], send_sem=ids_send.at[1], recv_sem=ids_recv.at[1],
            device_id=plane[n], device_id_type=MESH)

    for n in range(1, 8):
        line_copy(n).start()
    passing[:, 0] = outbox[0]

    first = pltpu.make_async_remote_copy(
        src_ref=outbox.at[pl.ds(1, 7)], dst_ref=outbox.at[pl.ds(1, 7)], send_sem=ids_send.at[0],
        recv_sem=ids_recv.at[0], device_id=line[1], device_id_type=MESH)
    second = pltpu.make_async_remote_copy(
        src_ref=passing.at[pl.ds(1, 15)], dst_ref=passing.at[pl.ds(1, 15)], send_sem=ids_send.at[1],
        recv_sem=ids_recv.at[1], device_id=plane[1], device_id_type=MESH)
    first.wait_recv()
    for n in range(1, 16):
        plane_copy(n).start()
    own = pltpu.make_async_copy(passing.at[0], ids.at[pl.ds(0, 8)], smem_sem)
    own.start()

    def device(kind, da, db, dy, core, sign):
        dx, dz = da + kind * (db - da), db + kind * (da - db)
        return (lax.rem(x + 4 + sign * dx, 4) * 4 + lax.rem(z + 4 + sign * dz, 4), lax.rem(y + 4 + sign * dy, 4) * 2 + core)

    def line_at(t, n):
        return (0, n, t) if n < 3 else (t, 3, 0)

    def line_order(slot):
        dy, dc, dx, dz = slot // 32, slot // 16 % 2, slot // 4 % 4, slot % 4
        da, db = dx + c * (dz - dx), dz + c * (dx - dz)
        on_y = db == 3
        t, member = jnp.where(on_y, da, dy), jnp.where(on_y, dy, da)
        return (t * 4 + db) * 2 + member // 2, member % 2 * 2 + (c + dc) % 2

    bags = dot(all_oh, vbag[...], NT_DIMS)
    bags = jnp.where(lan // CAP == line_order(sub)[1], bags, 0.0).astype(BF16)
    pick = (line_order(lan[:32])[0] == sub[:32]).astype(F32).astype(BF16)
    mybags[...] = dot(pick, bags).astype(I32).reshape(32, 1, NDEV)
    for cp in loads[2:]:
        cp.wait()
    dense = dense_ref[...]
    hidden = lax.dot_general(dense, wd[...], NN_DIMS, precision=lax.Precision.HIGHEST,
                             preferred_element_type=F32) + bias[...]
    for cp in tab_loads:
        cp.wait()

    second.wait_recv()

    def bags_copy(t, n):
        return pltpu.make_async_remote_copy(
            src_ref=mybags.at[pl.ds((t * 4 + n) * 2, 2)], dst_ref=linebags.at[pl.ds((t * 4 + n) * 2, 2)],
            send_sem=bag_send, recv_sem=bag_recv, device_id=device(c, *line_at(t, n), c, 1), device_id_type=MESH)

    for t in range(4):
        for n in range(4):
            if t or n:
                bags_copy(t, n).start()
    linebags[0:2] = mybags[0:2]
    own.wait()
    def block(dst, at, e):
        for j in range(CAP):
            dst[(*at, slice(j, j + 1))] = tab[pl.ds(ids[e, 0, j], 1), :]

    def entry(kind, other, da, db, dy):
        return (da * (4 - 3 * kind) + db * (1 + 3 * kind)) * 8 + dy * 2 + other

    def rows_copy(src, dst, t, peer):
        return pltpu.make_async_remote_copy(
            src_ref=src, dst_ref=dst, send_sem=row_send, recv_sem=row_recv.at[t], device_id=peer, device_id_type=MESH)

    @pl.loop(0, 4)
    def _(t):
        for other in range(2):
            kind = c + other * (1 - 2 * c)
            base = (other * 4 + t) * 4

            def gather(m, dst, at):
                for n in range(4):
                    da, db, dy = (m, n, t) if n < 3 else (t, 3, m)
                    block(dst, at(m, n), entry(kind, other, da, db, dy))

            def send(m):
                if m == 0:
                    rows_copy(stage.at[base], agg.at[t, :, 0, c], t, (my_row, y * 2 + kind)).start()
                    return
                rows_copy(stage.at[base + m, pl.ds(0, 3)], agg.at[t, pl.ds(0, 3), m, c], t,
                          device(kind, m, 0, 0, kind, -1)).start()
                rows_copy(stage.at[base + m, 3], agg.at[t, 3, m, c], t, device(kind, 0, 0, m, kind, -1)).start()

            if other == 0:
                gather(0, agg, lambda m, n: (t, n, m, c))

            @pl.loop(1 - other, 4)
            def _(m):
                gather(m, stage, lambda m, n: (base + m, n))
            for m in range(1 - other, 4):
                send(m)

    def count(blocks, sem):
        return pltpu.make_async_remote_copy(
            src_ref=stage.at[pl.ds(0, blocks)], dst_ref=stage.at[pl.ds(0, blocks)], send_sem=sem, recv_sem=sem,
            device_id=line[1], device_id_type=MESH)

    all_bags = pltpu.make_async_remote_copy(
        src_ref=mybags.at[pl.ds(2, 30)], dst_ref=linebags.at[pl.ds(2, 30)], send_sem=bag_send, recv_sem=bag_recv,
        device_id=line[1], device_id_type=MESH)
    all_bags.wait_recv()
    want = lax.broadcasted_iota(I32, (BAGS, NDEV), 0) + 1

    def sum_copy(t, n):
        return pltpu.make_async_remote_copy(
            src_ref=sums.at[t * 4 + n], dst_ref=parts.at[t * 4 + n], send_sem=sum_send, recv_sem=sum_recv.at[t],
            device_id=device(c, *line_at(t, n), c, -1), device_id_type=MESH)

    def sums_of(t):
        begin = 1 if t == 0 else t * 4
        span = pl.ds(begin, t * 4 + 4 - begin)
        return pltpu.make_async_remote_copy(
            src_ref=sums.at[span], dst_ref=parts.at[span], send_sem=sum_send, recv_sem=sum_recv.at[t],
            device_id=line[1], device_id_type=MESH)

    for t in range(4):
        count(7, row_recv.at[t]).wait_recv()
        for n in range(4):
            at = (t * 4 + n) * 2
            w = jnp.concatenate([(want == linebags[at + h]).astype(F32) for h in range(2)], axis=1).astype(BF16)
            hi, lo = split2(agg[t, n].reshape(8 * CAP, E))
            part = dot(w, hi) + dot(w, lo)
            if t or n:
                sums[t * 4 + n] = part
                sum_copy(t, n).start()
            else:
                parts[0] = part

    total = jnp.zeros((BAGS, E), F32)
    for t in range(4):
        sums_of(t).wait_recv()
        for n in range(4):
            total = total + parts[t * 4 + n]

    feats = [dense] + [total[t * 16:(t + 1) * 16] for t in range(NT)]
    for t in range(NT):
        pooled_out[:, t, :] = feats[t + 1]
    k = 0
    for a in range(NT + 1):
        for b in range(a + 1, NT + 1):
            d = jnp.sum(feats[a] * feats[b], axis=-1, keepdims=True)
            hidden = hidden + d * wp[k:k + 1, :]
            k += 1
    hidden_out[...] = jnp.maximum(hidden, 0.0)

    first.wait_send()
    second.wait_send()
    all_bags.wait_send()
    count(28, row_send).wait_send()
    pltpu.make_async_remote_copy(
        src_ref=sums.at[pl.ds(1, 15)], dst_ref=parts.at[pl.ds(1, 15)], send_sem=sum_send, recv_sem=sum_recv.at[0],
        device_id=line[1], device_id_type=MESH).wait_send()


def put_out(pooled, hidden, pooled_out, hidden_out, sems):
    copies = [pltpu.make_async_copy(pooled, pooled_out, sems.at[0]), pltpu.make_async_copy(hidden, hidden_out, sems.at[1])]
    for cp in copies:
        cp.start()
    for cp in copies:
        cp.wait()


def shards(bag_index, bag_length, emb_tables, dense_feats, w_dense, w_pair, top_bias):
    rows = NT * emb_tables.shape[1]
    hidden = w_dense.shape[1]
    slots = 16 * NDEV
    vmem, hbm = pl.BlockSpec(memory_space=pltpu.VMEM), pl.BlockSpec(memory_space=pltpu.HBM)
    outs = (jax.ShapeDtypeStruct((16, NT, E), F32), jax.ShapeDtypeStruct((16, hidden), F32))
    found = pl.pallas_call(
        kernel,
        out_shape=outs,
        in_specs=[hbm] * 7,
        out_specs=(vmem, vmem),
        scratch_shapes=[
            pltpu.VMEM((16, NDEV), I32),
            pltpu.VMEM((NT, 16), I32),
            pltpu.VMEM((rows, E), F32),
            pltpu.VMEM((16, E), F32),
            pltpu.VMEM(w_dense.shape, F32),
            pltpu.VMEM(w_pair.shape, F32),
            pltpu.VMEM((1, hidden), F32),
            pltpu.VMEM((NDEV, slots), BF16),
            pltpu.VMEM((CAP, slots), BF16),
            pltpu.VMEM((CAP, slots), BF16),
            pltpu.VMEM((NDEV, slots), BF16),
            pltpu.VMEM((8, 16, 1, CAP), I32),
            pltpu.VMEM((16, 8, 1, CAP), I32),
            pltpu.SMEM((NDEV, 1, CAP), I32),
            pltpu.VMEM((32, 1, NDEV), I32),
            pltpu.VMEM((32, 1, NDEV), I32),
            pltpu.VMEM((32, 4, CAP, E), F32),
            pltpu.VMEM((4, 4, 4, 2, CAP, E), F32),
            pltpu.VMEM((16, BAGS, E), F32),
            pltpu.VMEM((16, BAGS, E), F32),
            pltpu.SemaphoreType.DMA((6,)),
            pltpu.SemaphoreType.DMA((TAB_PARTS,)),
            pltpu.SemaphoreType.DMA((2,)),
            pltpu.SemaphoreType.DMA((2,)),
            pltpu.SemaphoreType.DMA,
            pltpu.SemaphoreType.DMA,
            pltpu.SemaphoreType.DMA,
            pltpu.SemaphoreType.DMA,
            pltpu.SemaphoreType.DMA((4,)),
            pltpu.SemaphoreType.DMA,
            pltpu.SemaphoreType.DMA((4,)),
        ],
        compiler_params=pltpu.CompilerParams(
            collective_id=0, has_side_effects=True, vmem_limit_bytes=40 * 1024 * 1024),
    )(*[pltpu.with_memory_space_constraint(a, pltpu.HBM) for a in (
        bag_index, bag_length.T, emb_tables.reshape(rows, E), dense_feats, w_dense, w_pair,
        top_bias.reshape(1, hidden))])
    return pl.pallas_call(
        put_out,
        out_shape=outs,
        in_specs=[vmem, vmem],
        out_specs=(hbm, hbm),
        scratch_shapes=[pltpu.SemaphoreType.DMA((2,))],
    )(*[pltpu.with_memory_space_constraint(a, pltpu.VMEM) for a in found])


def solution(mesh):
    samples = P(("rows", "cols"), None)
    in_specs = (samples, samples, P(None, ("rows", "cols"), None), samples, P(), P(), P())
    out_specs = (P(("rows", "cols"), None, None), samples)
    return jax.shard_map(shards, mesh=mesh, in_specs=in_specs, out_specs=out_specs, check_vma=False)
```

```python
import functools

import jax
import jax.numpy as jnp
from jax import lax
from jax.experimental import pallas as pl
from jax.experimental.pallas import tpu as pltpu
from jax.sharding import PartitionSpec as P

NT = 4
L = 32
E = 128
NDEV = 128
CAP = 32
BAGS = 64
TAB_PARTS = 8
MESH = pl.DeviceIdType.MESH
F32, BF16, I32 = jnp.float32, jnp.bfloat16, jnp.int32
NT_DIMS = (((1,), (1,)), ((), ()))
TN_DIMS = (((0,), (0,)), ((), ()))
NN_DIMS = (((1,), (0,)), ((), ()))


def dot(a, b, dims=NN_DIMS):
    return lax.dot_general(a, b, dims, preferred_element_type=F32)


def split2(v):
    hi = v.astype(BF16)
    return hi, (v - hi.astype(F32)).astype(BF16)


def position():
    r, c = lax.axis_index("rows"), lax.axis_index("cols")
    return lax.div(r, 4), lax.rem(r, 4), lax.div(c, 2), lax.rem(c, 2)


def around(at, n, sign=1):
    return [lax.rem(at + n + sign * d, n) for d in range(n)]


def kernel(idx_hbm, len_hbm, tab_hbm, dense_hbm, wd_hbm, wp_hbm, bias_hbm, pooled_out, hidden_out,
           idx_ref, len_ref, tab, dense_ref, wd, wp, bias, ohs, vcode, vbag, outbox, passing, ids, mybags, linebags, stage, agg, sums, parts,
           load_sem, tab_sem, ids_send, ids_recv, smem_sem, bag_send, bag_recv, row_send, row_recv, sum_send, sum_recv):
    me = position()
    loads = [pltpu.make_async_copy(s, d, load_sem.at[n]) for n, (s, d) in
             enumerate(((idx_hbm, idx_ref), (len_hbm, len_ref), (dense_hbm, dense_ref), (wd_hbm, wd), (wp_hbm, wp),
                        (bias_hbm, bias)))]
    part = tab.shape[0] // TAB_PARTS
    tab_loads = [pltpu.make_async_copy(tab_hbm.at[pl.ds(n * part, part)], tab.at[pl.ds(n * part, part)], tab_sem.at[n])
                 for n in range(TAB_PARTS)]

    for cp in loads[:2] + tab_loads + loads[2:]:
        cp.start()
    barrier = pltpu.get_barrier_semaphore()

    my_row, my_col = lax.axis_index("rows"), lax.axis_index("cols")
    xs, zs, ys, cs = [around(at, n) for at, n in zip(me, (4, 4, 4, 2))]
    line = [(my_row, y * 2 + c) for y in ys for c in cs]
    plane = [(x * 4 + z, my_col) for x in xs for z in zs]
    for peer in plane[1:] + line[1:]:
        pl.semaphore_signal(barrier, inc=1, device_id=peer, device_id_type=MESH)


    for cp in loads[:2]:
        cp.wait()
    idx = idx_ref[...]
    local_rows = tab.shape[0] // NT
    lane = lax.broadcasted_iota(I32, (16, NDEV), 1)
    table_of = lane // L
    of_table = (lax.broadcasted_iota(I32, (NT, NDEV), 1) // L == lax.broadcasted_iota(I32, (NT, NDEV), 0)).astype(F32)
    limit = dot(len_ref[...].astype(F32), of_table, TN_DIMS).astype(I32)
    live = lane % L < limit
    owner = idx // local_rows
    code = table_of * local_rows + idx % local_rows
    ox, oz, oy, oc = owner // 32, owner // 8 % 4, owner // 2 % 4, owner % 2
    x, z, y, c = me
    slot = (oy - y + 4) % 4 * 32 + (oc - c + 2) % 2 * 16 + (ox - x + 4) % 4 * 4 + (oz - z + 4) % 4
    rel = jnp.where(live, slot, -1)
    bag = lax.broadcasted_iota(I32, (16, NDEV), 0) + 16 * table_of + 1
    sub = lax.broadcasted_iota(I32, (NDEV, NDEV), 0)
    lan = lax.broadcasted_iota(I32, (NDEV, NDEV), 1)
    before = jnp.concatenate([(sub < lan).astype(F32), jnp.ones((NDEV, NDEV), F32)], axis=1).astype(BF16)
    code_hi, code_lo, bag = (code // 256).astype(F32), (code % 256).astype(F32), bag.astype(F32)
    carry = jnp.zeros((NDEV, NDEV), F32)
    ranks = []
    for r in range(16):
        oh = (sub == rel[r:r + 1, :]).astype(F32)
        ohb = oh.astype(BF16)
        counts = dot(ohb, before)
        rank = jnp.sum(oh * (counts[:, :NDEV] + carry), axis=0, keepdims=True).astype(I32)
        carry = carry + counts[:, NDEV:]
        cols = slice(r * NDEV, (r + 1) * NDEV)
        here = sub[:CAP] == rank
        ohs[:, cols] = ohb
        vcode[:CAP, cols] = jnp.where(here, code_hi[r:r + 1], 0.0).astype(BF16)
        vcode[CAP:, cols] = jnp.where(here, code_lo[r:r + 1], 0.0).astype(BF16)
        ranks.append(rank)
    all_oh = ohs[...]
    box = dot(all_oh, vcode[...], NT_DIMS)
    box = box[:, :CAP] * 256.0 + box[:, CAP:]
    outbox[...] = jnp.clip(box.astype(I32), 0, tab.shape[0] - 1).reshape(8, 16, 1, CAP)

    pl.semaphore_wait(barrier, 22)

    def line_copy(n):
        return pltpu.make_async_remote_copy(
            src_ref=outbox.at[n], dst_ref=passing.at[:, n], send_sem=ids_send.at[0], recv_sem=ids_recv.at[0],
            device_id=line[n], device_id_type=MESH)

    def plane_copy(n):
        return pltpu.make_async_remote_copy(
            src_ref=passing.at[n], dst_ref=ids.at[pl.ds(n * 8, 8)], send_sem=ids_send.at[1], recv_sem=ids_recv.at[1],
            device_id=plane[n], device_id_type=MESH)

    for n in range(1, 8):
        line_copy(n).start()
    passing[:, 0] = outbox[0]

    first = pltpu.make_async_remote_copy(
        src_ref=outbox.at[pl.ds(1, 7)], dst_ref=outbox.at[pl.ds(1, 7)], send_sem=ids_send.at[0],
        recv_sem=ids_recv.at[0], device_id=line[1], device_id_type=MESH)
    second = pltpu.make_async_remote_copy(
        src_ref=passing.at[pl.ds(1, 15)], dst_ref=passing.at[pl.ds(1, 15)], send_sem=ids_send.at[1],
        recv_sem=ids_recv.at[1], device_id=plane[1], device_id_type=MESH)
    first.wait_recv()
    for n in range(1, 16):
        plane_copy(n).start()
    own = pltpu.make_async_copy(passing.at[0], ids.at[pl.ds(0, 8)], smem_sem)
    own.start()

    def device(kind, da, db, dy, core, sign):
        dx, dz = da + kind * (db - da), db + kind * (da - db)
        return (lax.rem(x + 4 + sign * dx, 4) * 4 + lax.rem(z + 4 + sign * dz, 4), lax.rem(y + 4 + sign * dy, 4) * 2 + core)

    def line_at(t, n):
        return (0, n, t) if n < 3 else (t, 3, 0)

    def line_order(slot):
        dy, dc, dx, dz = slot // 32, slot // 16 % 2, slot // 4 % 4, slot % 4
        da, db = dx + c * (dz - dx), dz + c * (dx - dz)
        on_y = db == 3
        t, member = jnp.where(on_y, da, dy), jnp.where(on_y, dy, da)
        return (t * 4 + db) * 2 + member // 2, member % 2 * 2 + (c + dc) % 2

    for r in range(16):
        vbag[:, r * NDEV:(r + 1) * NDEV] = jnp.where(sub % CAP == ranks[r], bag[r:r + 1], 0.0).astype(BF16)
    bags = dot(all_oh, vbag[...], NT_DIMS)
    bags = jnp.where(lan // CAP == line_order(sub)[1], bags, 0.0).astype(BF16)
    pick = (line_order(lan[:32])[0] == sub[:32]).astype(F32).astype(BF16)
    mybags[...] = dot(pick, bags).astype(I32).reshape(32, 1, NDEV)
    for cp in loads[2:]:
        cp.wait()
    dense = dense_ref[...]
    hidden = lax.dot_general(dense, wd[...], NN_DIMS, precision=lax.Precision.HIGHEST,
                             preferred_element_type=F32) + bias[...]
    for cp in tab_loads:
        cp.wait()

    second.wait_recv()

    def bags_copy(t, n):
        return pltpu.make_async_remote_copy(
            src_ref=mybags.at[pl.ds((t * 4 + n) * 2, 2)], dst_ref=linebags.at[pl.ds((t * 4 + n) * 2, 2)],
            send_sem=bag_send, recv_sem=bag_recv, device_id=device(c, *line_at(t, n), c, 1), device_id_type=MESH)

    for t in range(4):
        for n in range(4):
            if t or n:
                bags_copy(t, n).start()
    linebags[0:2] = mybags[0:2]
    own.wait()
    def block(dst, at, e):
        for j in range(CAP):
            dst[(*at, slice(j, j + 1))] = tab[pl.ds(ids[e, 0, j], 1), :]

    def entry(kind, other, da, db, dy):
        return (da * (4 - 3 * kind) + db * (1 + 3 * kind)) * 8 + dy * 2 + other

    def rows_copy(src, dst, t, peer):
        return pltpu.make_async_remote_copy(
            src_ref=src, dst_ref=dst, send_sem=row_send, recv_sem=row_recv.at[t], device_id=peer, device_id_type=MESH)

    def push(t):
        def gather(kind, other, m, dst, at):
            for n in range(4):
                da, db, dy = (m, n, t) if n < 3 else (t, 3, m)
                block(dst, at(n), entry(kind, other, da, db, dy))

        @pl.loop(0, 6)
        def _(i):
            other, m = lax.rem(i, 2), lax.div(i, 2) + 1
            kind = c + other * (1 - 2 * c)
            at = (other * 4 + t) * 4 + m
            gather(kind, other, m, stage, lambda n: (at, n))
            rows_copy(stage.at[at, pl.ds(0, 3)], agg.at[t, pl.ds(0, 3), m, c], t,
                      device(kind, m, 0, 0, kind, -1)).start()
            rows_copy(stage.at[at, 3], agg.at[t, 3, m, c], t, device(kind, 0, 0, m, kind, -1)).start()

        gather(1 - c, 1, 0, stage, lambda n: ((4 + t) * 4, n))
        rows_copy(stage.at[(4 + t) * 4], agg.at[t, :, 0, c], t, (my_row, y * 2 + 1 - c)).start()
        gather(c, 0, 0, agg, lambda n: (t, n, 0, c))

    def count(blocks, sem):
        return pltpu.make_async_remote_copy(
            src_ref=stage.at[pl.ds(0, blocks)], dst_ref=stage.at[pl.ds(0, blocks)], send_sem=sem, recv_sem=sem,
            device_id=line[1], device_id_type=MESH)

    all_bags = pltpu.make_async_remote_copy(
        src_ref=mybags.at[pl.ds(2, 30)], dst_ref=linebags.at[pl.ds(2, 30)], send_sem=bag_send, recv_sem=bag_recv,
        device_id=line[1], device_id_type=MESH)
    want = lax.broadcasted_iota(I32, (BAGS, NDEV), 0) + 1

    def sum_copy(t, n):
        return pltpu.make_async_remote_copy(
            src_ref=sums.at[t * 4 + n], dst_ref=parts.at[t * 4 + n], send_sem=sum_send, recv_sem=sum_recv.at[t],
            device_id=device(c, *line_at(t, n), c, -1), device_id_type=MESH)

    def sums_of(t):
        begin = 1 if t == 0 else t * 4
        span = pl.ds(begin, t * 4 + 4 - begin)
        return pltpu.make_async_remote_copy(
            src_ref=sums.at[span], dst_ref=parts.at[span], send_sem=sum_send, recv_sem=sum_recv.at[t],
            device_id=line[1], device_id_type=MESH)

    def pool(t):
        count(7, row_recv.at[t]).wait_recv()
        for n in (2, 1, 3, 0):
            at = (t * 4 + n) * 2
            w = jnp.concatenate([(want == linebags[at + h]).astype(F32) for h in range(2)], axis=1).astype(BF16)
            hi, lo = split2(agg[t, n].reshape(8 * CAP, E))
            part = dot(w, hi) + dot(w, lo)
            if t or n:
                sums[t * 4 + n] = part
                sum_copy(t, n).start()
            else:
                parts[0] = part

    order = (2, 1, 3, 0)
    for t in order:
        push(t)
    all_bags.wait_recv()
    for t in order:
        pool(t)

    total = jnp.zeros((BAGS, E), F32)
    for t in order:
        sums_of(t).wait_recv()
        for n in range(4):
            total = total + parts[t * 4 + n]

    feats = [dense] + [total[t * 16:(t + 1) * 16] for t in range(NT)]
    for t in range(NT):
        pooled_out[:, t, :] = feats[t + 1]
    k = 0
    for a in range(NT + 1):
        for b in range(a + 1, NT + 1):
            d = jnp.sum(feats[a] * feats[b], axis=-1, keepdims=True)
            hidden = hidden + d * wp[k:k + 1, :]
            k += 1
    hidden_out[...] = jnp.maximum(hidden, 0.0)

    first.wait_send()
    second.wait_send()
    all_bags.wait_send()
    count(28, row_send).wait_send()
    pltpu.make_async_remote_copy(
        src_ref=sums.at[pl.ds(1, 15)], dst_ref=parts.at[pl.ds(1, 15)], send_sem=sum_send, recv_sem=sum_recv.at[0],
        device_id=line[1], device_id_type=MESH).wait_send()


def put_out(pooled, hidden, pooled_out, hidden_out, sems):
    copies = [pltpu.make_async_copy(pooled, pooled_out, sems.at[0]), pltpu.make_async_copy(hidden, hidden_out, sems.at[1])]
    for cp in copies:
        cp.start()
    for cp in copies:
        cp.wait()


def shards(bag_index, bag_length, emb_tables, dense_feats, w_dense, w_pair, top_bias):
    rows = NT * emb_tables.shape[1]
    hidden = w_dense.shape[1]
    slots = 16 * NDEV
    vmem, hbm = pl.BlockSpec(memory_space=pltpu.VMEM), pl.BlockSpec(memory_space=pltpu.HBM)
    outs = (jax.ShapeDtypeStruct((16, NT, E), F32), jax.ShapeDtypeStruct((16, hidden), F32))
    found = pl.pallas_call(
        kernel,
        out_shape=outs,
        in_specs=[hbm] * 7,
        out_specs=(vmem, vmem),
        scratch_shapes=[
            pltpu.VMEM((16, NDEV), I32),
            pltpu.VMEM((NT, 16), I32),
            pltpu.VMEM((rows, E), F32),
            pltpu.VMEM((16, E), F32),
            pltpu.VMEM(w_dense.shape, F32),
            pltpu.VMEM(w_pair.shape, F32),
            pltpu.VMEM((1, hidden), F32),
            pltpu.VMEM((NDEV, slots), BF16),
            pltpu.VMEM((2 * CAP, slots), BF16),
            pltpu.VMEM((NDEV, slots), BF16),
            pltpu.VMEM((8, 16, 1, CAP), I32),
            pltpu.VMEM((16, 8, 1, CAP), I32),
            pltpu.SMEM((NDEV, 1, CAP), I32),
            pltpu.VMEM((32, 1, NDEV), I32),
            pltpu.VMEM((32, 1, NDEV), I32),
            pltpu.VMEM((32, 4, CAP, E), F32),
            pltpu.VMEM((4, 4, 4, 2, CAP, E), F32),
            pltpu.VMEM((16, BAGS, E), F32),
            pltpu.VMEM((16, BAGS, E), F32),
            pltpu.SemaphoreType.DMA((6,)),
            pltpu.SemaphoreType.DMA((TAB_PARTS,)),
            pltpu.SemaphoreType.DMA((2,)),
            pltpu.SemaphoreType.DMA((2,)),
            pltpu.SemaphoreType.DMA,
            pltpu.SemaphoreType.DMA,
            pltpu.SemaphoreType.DMA,
            pltpu.SemaphoreType.DMA,
            pltpu.SemaphoreType.DMA((4,)),
            pltpu.SemaphoreType.DMA,
            pltpu.SemaphoreType.DMA((4,)),
        ],
        compiler_params=pltpu.CompilerParams(
            collective_id=0, has_side_effects=True, vmem_limit_bytes=40 * 1024 * 1024),
    )(*[pltpu.with_memory_space_constraint(a, pltpu.HBM) for a in (
        bag_index, bag_length.T, emb_tables.reshape(rows, E), dense_feats, w_dense, w_pair,
        top_bias.reshape(1, hidden))])
    return pl.pallas_call(
        put_out,
        out_shape=outs,
        in_specs=[vmem, vmem],
        out_specs=(hbm, hbm),
        scratch_shapes=[pltpu.SemaphoreType.DMA((2,))],
    )(*[pltpu.with_memory_space_constraint(a, pltpu.VMEM) for a in found])


def solution(mesh):
    samples = P(("rows", "cols"), None)
    in_specs = (samples, samples, P(None, ("rows", "cols"), None), samples, P(), P(), P())
    out_specs = (P(("rows", "cols"), None, None), samples)
    return jax.shard_map(shards, mesh=mesh, in_specs=in_specs, out_specs=out_specs, check_vma=False)
```

```python
import functools

import jax
import jax.numpy as jnp
from jax import lax
from jax.experimental import pallas as pl
from jax.experimental.pallas import tpu as pltpu
from jax.sharding import PartitionSpec as P

NT = 4
L = 32
E = 128
NDEV = 128
CAP = 32
BAGS = 64
TAB_PARTS = 8
EARLY = 2
PLANE_PAIRS = ((0, 1), (0, 3), (0, 2), (1, 1), (1, 3), (3, 3), (1, 2), (2, 3), (2, 2), (0, 0))
MESH = pl.DeviceIdType.MESH
F32, BF16, I32 = jnp.float32, jnp.bfloat16, jnp.int32
NT_DIMS = (((1,), (1,)), ((), ()))
TN_DIMS = (((0,), (0,)), ((), ()))
NN_DIMS = (((1,), (0,)), ((), ()))


def dot(a, b, dims=NN_DIMS):
    return lax.dot_general(a, b, dims, preferred_element_type=F32)


def split2(v):
    hi = v.astype(BF16)
    return hi, (v - hi.astype(F32)).astype(BF16)


def position():
    r, c = lax.axis_index("rows"), lax.axis_index("cols")
    return lax.div(r, 4), lax.rem(r, 4), lax.div(c, 2), lax.rem(c, 2)


def around(at, n, sign=1):
    return [lax.rem(at + n + sign * d, n) for d in range(n)]


def kernel(idx_hbm, len_hbm, tab_hbm, dense_hbm, wd_hbm, wp_hbm, bias_hbm, pooled_out, hidden_out,
           idx_ref, len_ref, tab, dense_ref, wd, wp, bias, ohs, vcode, vbag, outbox, passing, ids, mybags, linebags, stage, agg, sums, parts,
           load_sem, tab_sem, ids_send, ids_recv, smem_sem, bag_send, bag_recv, row_send, row_recv, sum_send, sum_recv):
    me = position()
    loads = [pltpu.make_async_copy(s, d, load_sem.at[n]) for n, (s, d) in
             enumerate(((idx_hbm, idx_ref), (len_hbm, len_ref), (dense_hbm, dense_ref), (wd_hbm, wd), (wp_hbm, wp),
                        (bias_hbm, bias)))]
    part = tab.shape[0] // TAB_PARTS
    tab_loads = [pltpu.make_async_copy(tab_hbm.at[pl.ds(n * part, part)], tab.at[pl.ds(n * part, part)], tab_sem.at[n])
                 for n in range(TAB_PARTS)]

    for cp in loads[:2] + tab_loads + loads[2:]:
        cp.start()
    barrier = pltpu.get_barrier_semaphore()

    my_row, my_col = lax.axis_index("rows"), lax.axis_index("cols")
    xs, zs, ys, cs = [around(at, n) for at, n in zip(me, (4, 4, 4, 2))]
    line = [(my_row, y * 2 + c) for y in ys for c in cs]
    plane = [(x * 4 + z, my_col) for x in xs for z in zs]
    for peer in plane[1:] + line[1:]:
        pl.semaphore_signal(barrier, inc=1, device_id=peer, device_id_type=MESH)


    for cp in loads[:2]:
        cp.wait()
    idx = idx_ref[...]
    local_rows = tab.shape[0] // NT
    lane = lax.broadcasted_iota(I32, (16, NDEV), 1)
    table_of = lane // L
    of_table = (lax.broadcasted_iota(I32, (NT, NDEV), 1) // L == lax.broadcasted_iota(I32, (NT, NDEV), 0)).astype(F32)
    limit = dot(len_ref[...].astype(F32), of_table, TN_DIMS).astype(I32)
    live = lane % L < limit
    owner = idx // local_rows
    code = table_of * local_rows + idx % local_rows
    ox, oz, oy, oc = owner // 32, owner // 8 % 4, owner // 2 % 4, owner % 2
    x, z, y, c = me
    slot = (oy - y + 4) % 4 * 32 + (oc - c + 2) % 2 * 16 + (ox - x + 4) % 4 * 4 + (oz - z + 4) % 4
    rel = jnp.where(live, slot, -1)
    bag = lax.broadcasted_iota(I32, (16, NDEV), 0) + 16 * table_of + 1
    sub = lax.broadcasted_iota(I32, (NDEV, NDEV), 0)
    lan = lax.broadcasted_iota(I32, (NDEV, NDEV), 1)
    before = jnp.concatenate([(sub < lan).astype(F32), jnp.ones((NDEV, NDEV), F32)], axis=1).astype(BF16)
    code_hi, code_lo, bag = (code // 256).astype(F32), (code % 256).astype(F32), bag.astype(F32)
    carry = jnp.zeros((NDEV, NDEV), F32)
    ranks = []
    for r in range(16):
        oh = (sub == rel[r:r + 1, :]).astype(F32)
        ohb = oh.astype(BF16)
        counts = dot(ohb, before)
        rank = jnp.sum(oh * (counts[:, :NDEV] + carry), axis=0, keepdims=True).astype(I32)
        carry = carry + counts[:, NDEV:]
        cols = slice(r * NDEV, (r + 1) * NDEV)
        here = sub[:CAP] == rank
        ohs[:, cols] = ohb
        vcode[:CAP, cols] = jnp.where(here, code_hi[r:r + 1], 0.0).astype(BF16)
        vcode[CAP:, cols] = jnp.where(here, code_lo[r:r + 1], 0.0).astype(BF16)
        ranks.append(rank)
    all_oh = ohs[...]
    box = dot(all_oh, vcode[...], NT_DIMS)
    box = box[:, :CAP] * 256.0 + box[:, CAP:]
    outbox[...] = jnp.clip(box.astype(I32), 0, tab.shape[0] - 1).reshape(8, 16, 1, CAP)

    pl.semaphore_wait(barrier, 22)

    def line_copy(n):
        return pltpu.make_async_remote_copy(
            src_ref=outbox.at[n], dst_ref=passing.at[:, n], send_sem=ids_send.at[0], recv_sem=ids_recv.at[0],
            device_id=line[n], device_id_type=MESH)

    def plane_copy(n):
        return pltpu.make_async_remote_copy(
            src_ref=passing.at[n], dst_ref=ids.at[pl.ds(n * 8, 8)], send_sem=ids_send.at[1], recv_sem=ids_recv.at[n],
            device_id=plane[n], device_id_type=MESH)

    for n in range(1, 8):
        line_copy(n).start()
    passing[:, 0] = outbox[0]

    first = pltpu.make_async_remote_copy(
        src_ref=outbox.at[pl.ds(1, 7)], dst_ref=outbox.at[pl.ds(1, 7)], send_sem=ids_send.at[0],
        recv_sem=ids_recv.at[0], device_id=line[1], device_id_type=MESH)
    first.wait_recv()
    for n in range(1, 16):
        plane_copy(n).start()
    own = pltpu.make_async_copy(passing.at[0], ids.at[pl.ds(0, 8)], smem_sem)
    own.start()

    def device(kind, da, db, dy, core, sign):
        dx, dz = da + kind * (db - da), db + kind * (da - db)
        return (lax.rem(x + 4 + sign * dx, 4) * 4 + lax.rem(z + 4 + sign * dz, 4), lax.rem(y + 4 + sign * dy, 4) * 2 + core)

    def line_at(t, n):
        return (0, n, t) if n < 3 else (t, 3, 0)

    def line_order(slot):
        dy, dc, dx, dz = slot // 32, slot // 16 % 2, slot // 4 % 4, slot % 4
        da, db = dx + c * (dz - dx), dz + c * (dx - dz)
        on_y = db == 3
        t, member = jnp.where(on_y, da, dy), jnp.where(on_y, dy, da)
        return (t * 4 + db) * 2 + member // 2, member % 2 * 2 + (c + dc) % 2

    for r in range(16):
        vbag[:, r * NDEV:(r + 1) * NDEV] = jnp.where(sub % CAP == ranks[r], bag[r:r + 1], 0.0).astype(BF16)
    bags = dot(all_oh, vbag[...], NT_DIMS)
    bags = jnp.where(lan // CAP == line_order(sub)[1], bags, 0.0).astype(BF16)
    pick = (line_order(lan[:32])[0] == sub[:32]).astype(F32).astype(BF16)
    mybags[...] = dot(pick, bags).astype(I32).reshape(32, 1, NDEV)
    for cp in loads[2:]:
        cp.wait()
    dense = dense_ref[...]
    hidden = lax.dot_general(dense, wd[...], NN_DIMS, precision=lax.Precision.HIGHEST,
                             preferred_element_type=F32) + bias[...]
    for cp in tab_loads:
        cp.wait()


    def bags_copy(t, n):
        return pltpu.make_async_remote_copy(
            src_ref=mybags.at[pl.ds((t * 4 + n) * 2, 2)], dst_ref=linebags.at[pl.ds((t * 4 + n) * 2, 2)],
            send_sem=bag_send, recv_sem=bag_recv, device_id=device(c, *line_at(t, n), c, 1), device_id_type=MESH)

    def block(dst, at, e):
        for j in range(CAP):
            dst[(*at, slice(j, j + 1))] = tab[pl.ds(ids[e, 0, j], 1), :]

    def entry(kind, other, da, db, dy):
        return (da * (4 - 3 * kind) + db * (1 + 3 * kind)) * 8 + dy * 2 + other

    def rows_copy(src, dst, t, peer):
        return pltpu.make_async_remote_copy(
            src_ref=src, dst_ref=dst, send_sem=row_send, recv_sem=row_recv.at[t], device_id=peer, device_id_type=MESH)

    def push(t):
        def gather(kind, other, m, dst, at):
            for n in range(4):
                da, db, dy = (m, n, t) if n < 3 else (t, 3, m)
                block(dst, at(n), entry(kind, other, da, db, dy))

        @pl.loop(0, 6)
        def _(i):
            other, m = lax.rem(i, 2), lax.div(i, 2) + 1
            kind = c + other * (1 - 2 * c)
            at = (other * 4 + t) * 4 + m
            gather(kind, other, m, stage, lambda n: (at, n))
            rows_copy(stage.at[at, pl.ds(0, 3)], agg.at[t, pl.ds(0, 3), m, c], t,
                      device(kind, m, 0, 0, kind, -1)).start()
            rows_copy(stage.at[at, 3], agg.at[t, 3, m, c], t, device(kind, 0, 0, m, kind, -1)).start()

        gather(1 - c, 1, 0, stage, lambda n: ((4 + t) * 4, n))
        rows_copy(stage.at[(4 + t) * 4], agg.at[t, :, 0, c], t, (my_row, y * 2 + 1 - c)).start()
        gather(c, 0, 0, agg, lambda n: (t, n, 0, c))

    order = (2, 1, 3, 0)

    def push_early(ts):
        def one(t, other, m, n, dst, at):
            da, db, dy = (m, n, t) if n < 3 else (t, 3, m)
            block(dst, at, entry(c + other * (1 - 2 * c), other, da, db, dy))

        waited = set()
        for u, v in PLANE_PAIRS:
            for p in sorted({u * 4 + v, v * 4 + u} - waited):
                waited.add(p)
                if p:
                    plane_copy(p).wait_recv()
                else:
                    own.wait()
            if (u, v) == (0, 2):
                for q in order:
                    for n in (2, 1, 3, 0):
                        if q or n:
                            bags_copy(q, n).start()
                linebags[0:2] = mybags[0:2]
            spots = [(t, m, n) for t in ts for m, n in sorted({(u, v), (v, u)}) if n < 3]
            if 3 in (u, v):
                spots += [(t, m, 3) for t in ts if t == u + v - 3 for m in range(4)]
            for t, m, n in spots:
                if m:
                    @pl.loop(0, 2)
                    def _(other):
                        kind = c + other * (1 - 2 * c)
                        at = (other * 4 + t) * 4 + m
                        one(t, other, m, n, stage, (at, n))
                        away = (m, 0, 0) if n < 3 else (0, 0, m)
                        rows_copy(stage.at[at, n], agg.at[t, n, m, c], t, device(kind, *away, kind, -1)).start()
                else:
                    one(t, 1, 0, n, stage, ((4 + t) * 4, n))
                    rows_copy(stage.at[(4 + t) * 4, n], agg.at[t, n, 0, c], t, (my_row, y * 2 + 1 - c)).start()
                    one(t, 0, 0, n, agg, (t, n, 0, c))

    def count(blocks, sem):
        return pltpu.make_async_remote_copy(
            src_ref=stage.at[pl.ds(0, blocks)], dst_ref=stage.at[pl.ds(0, blocks)], send_sem=sem, recv_sem=sem,
            device_id=line[1], device_id_type=MESH)

    all_bags = pltpu.make_async_remote_copy(
        src_ref=mybags.at[pl.ds(2, 30)], dst_ref=linebags.at[pl.ds(2, 30)], send_sem=bag_send, recv_sem=bag_recv,
        device_id=line[1], device_id_type=MESH)
    want = lax.broadcasted_iota(I32, (BAGS, NDEV), 0) + 1

    def sum_copy(t, n):
        return pltpu.make_async_remote_copy(
            src_ref=sums.at[t * 4 + n], dst_ref=parts.at[t * 4 + n], send_sem=sum_send, recv_sem=sum_recv.at[t],
            device_id=device(c, *line_at(t, n), c, -1), device_id_type=MESH)

    def sums_of(t):
        begin = 1 if t == 0 else t * 4
        span = pl.ds(begin, t * 4 + 4 - begin)
        return pltpu.make_async_remote_copy(
            src_ref=sums.at[span], dst_ref=parts.at[span], send_sem=sum_send, recv_sem=sum_recv.at[t],
            device_id=line[1], device_id_type=MESH)

    def pool(t):
        count(7, row_recv.at[t]).wait_recv()
        for n in (2, 1, 3, 0):
            at = (t * 4 + n) * 2
            w = jnp.concatenate([(want == linebags[at + h]).astype(F32) for h in range(2)], axis=1).astype(BF16)
            hi, lo = split2(agg[t, n].reshape(8 * CAP, E))
            part = dot(w, hi) + dot(w, lo)
            if t or n:
                sums[t * 4 + n] = part
                sum_copy(t, n).start()
            else:
                parts[0] = part

    push_early(order[:EARLY])
    for t in order[EARLY:]:
        push(t)
    all_bags.wait_recv()
    for t in order:
        pool(t)

    total = jnp.zeros((BAGS, E), F32)
    for t in order:
        sums_of(t).wait_recv()
        for n in range(4):
            total = total + parts[t * 4 + n]

    feats = [dense] + [total[t * 16:(t + 1) * 16] for t in range(NT)]
    for t in range(NT):
        pooled_out[:, t, :] = feats[t + 1]
    k = 0
    for a in range(NT + 1):
        for b in range(a + 1, NT + 1):
            d = jnp.sum(feats[a] * feats[b], axis=-1, keepdims=True)
            hidden = hidden + d * wp[k:k + 1, :]
            k += 1
    hidden_out[...] = jnp.maximum(hidden, 0.0)

    first.wait_send()
    pltpu.make_async_remote_copy(
        src_ref=passing.at[pl.ds(1, 15)], dst_ref=passing.at[pl.ds(1, 15)], send_sem=ids_send.at[1],
        recv_sem=ids_recv.at[1], device_id=plane[1], device_id_type=MESH).wait_send()
    all_bags.wait_send()
    count(28, row_send).wait_send()
    pltpu.make_async_remote_copy(
        src_ref=sums.at[pl.ds(1, 15)], dst_ref=parts.at[pl.ds(1, 15)], send_sem=sum_send, recv_sem=sum_recv.at[0],
        device_id=line[1], device_id_type=MESH).wait_send()


def put_out(pooled, hidden, pooled_out, hidden_out, sems):
    copies = [pltpu.make_async_copy(pooled, pooled_out, sems.at[0]), pltpu.make_async_copy(hidden, hidden_out, sems.at[1])]
    for cp in copies:
        cp.start()
    for cp in copies:
        cp.wait()


def shards(bag_index, bag_length, emb_tables, dense_feats, w_dense, w_pair, top_bias):
    rows = NT * emb_tables.shape[1]
    hidden = w_dense.shape[1]
    slots = 16 * NDEV
    vmem, hbm = pl.BlockSpec(memory_space=pltpu.VMEM), pl.BlockSpec(memory_space=pltpu.HBM)
    outs = (jax.ShapeDtypeStruct((16, NT, E), F32), jax.ShapeDtypeStruct((16, hidden), F32))
    found = pl.pallas_call(
        kernel,
        out_shape=outs,
        in_specs=[hbm] * 7,
        out_specs=(vmem, vmem),
        scratch_shapes=[
            pltpu.VMEM((16, NDEV), I32),
            pltpu.VMEM((NT, 16), I32),
            pltpu.VMEM((rows, E), F32),
            pltpu.VMEM((16, E), F32),
            pltpu.VMEM(w_dense.shape, F32),
            pltpu.VMEM(w_pair.shape, F32),
            pltpu.VMEM((1, hidden), F32),
            pltpu.VMEM((NDEV, slots), BF16),
            pltpu.VMEM((2 * CAP, slots), BF16),
            pltpu.VMEM((NDEV, slots), BF16),
            pltpu.VMEM((8, 16, 1, CAP), I32),
            pltpu.VMEM((16, 8, 1, CAP), I32),
            pltpu.SMEM((NDEV, 1, CAP), I32),
            pltpu.VMEM((32, 1, NDEV), I32),
            pltpu.VMEM((32, 1, NDEV), I32),
            pltpu.VMEM((32, 4, CAP, E), F32),
            pltpu.VMEM((4, 4, 4, 2, CAP, E), F32),
            pltpu.VMEM((16, BAGS, E), F32),
            pltpu.VMEM((16, BAGS, E), F32),
            pltpu.SemaphoreType.DMA((6,)),
            pltpu.SemaphoreType.DMA((TAB_PARTS,)),
            pltpu.SemaphoreType.DMA((2,)),
            pltpu.SemaphoreType.DMA((16,)),
            pltpu.SemaphoreType.DMA,
            pltpu.SemaphoreType.DMA,
            pltpu.SemaphoreType.DMA,
            pltpu.SemaphoreType.DMA,
            pltpu.SemaphoreType.DMA((4,)),
            pltpu.SemaphoreType.DMA,
            pltpu.SemaphoreType.DMA((4,)),
        ],
        compiler_params=pltpu.CompilerParams(
            collective_id=0, has_side_effects=True, vmem_limit_bytes=40 * 1024 * 1024),
    )(*[pltpu.with_memory_space_constraint(a, pltpu.HBM) for a in (
        bag_index, bag_length.T, emb_tables.reshape(rows, E), dense_feats, w_dense, w_pair,
        top_bias.reshape(1, hidden))])
    return pl.pallas_call(
        put_out,
        out_shape=outs,
        in_specs=[vmem, vmem],
        out_specs=(hbm, hbm),
        scratch_shapes=[pltpu.SemaphoreType.DMA((2,))],
    )(*[pltpu.with_memory_space_constraint(a, pltpu.VMEM) for a in found])


def solution(mesh):
    samples = P(("rows", "cols"), None)
    in_specs = (samples, samples, P(None, ("rows", "cols"), None), samples, P(), P(), P())
    out_specs = (P(("rows", "cols"), None, None), samples)
    return jax.shard_map(shards, mesh=mesh, in_specs=in_specs, out_specs=out_specs, check_vma=False)
```

```python
import functools

import jax
import jax.numpy as jnp
from jax import lax
from jax.experimental import pallas as pl
from jax.experimental.pallas import tpu as pltpu
from jax.sharding import PartitionSpec as P

NT = 4
L = 32
E = 128
NDEV = 128
CAP = 32
BAGS = 64
TAB_PARTS = 8
NEAR, FAR = (0, 1, 3), 2
ORDER, EARLY = (2, 1, 3, 0), 2
FAR_LINES = {2: (2,), 1: (1,), 3: (3, 0), 0: ()}
PLANE_PAIRS = ((0, 0), (0, 1), (0, 3), (1, 1), (1, 3), (3, 3), (0, 2), (1, 2), (2, 3), (2, 2))
MESH = pl.DeviceIdType.MESH
F32, BF16, I32 = jnp.float32, jnp.bfloat16, jnp.int32
NT_DIMS = (((1,), (1,)), ((), ()))
TN_DIMS = (((0,), (0,)), ((), ()))
NN_DIMS = (((1,), (0,)), ((), ()))


def dot(a, b, dims=NN_DIMS):
    return lax.dot_general(a, b, dims, preferred_element_type=F32)


def split2(v):
    hi = v.astype(BF16)
    return hi, (v - hi.astype(F32)).astype(BF16)


def position():
    r, c = lax.axis_index("rows"), lax.axis_index("cols")
    return lax.div(r, 4), lax.rem(r, 4), lax.div(c, 2), lax.rem(c, 2)


def around(at, n, sign=1):
    return [lax.rem(at + n + sign * d, n) for d in range(n)]


def kernel(idx_hbm, len_hbm, tab_hbm, dense_hbm, wd_hbm, wp_hbm, bias_hbm, pooled_out, hidden_out,
           idx_ref, len_ref, tab, dense_ref, wd, wp, bias, ohs, vcode, vbag, outbox, passing, ids, mybags, bagpass, linebags, stage, agg, sums, parts,
           load_sem, tab_sem, ids_send, ids_recv, smem_sem, bag_send, bag_recv, row_send, row_recv, sum_send, sum_recv):
    me = position()
    loads = [pltpu.make_async_copy(s, d, load_sem.at[n]) for n, (s, d) in
             enumerate(((idx_hbm, idx_ref), (len_hbm, len_ref), (dense_hbm, dense_ref), (wd_hbm, wd), (wp_hbm, wp),
                        (bias_hbm, bias)))]
    part = tab.shape[0] // TAB_PARTS
    tab_loads = [pltpu.make_async_copy(tab_hbm.at[pl.ds(n * part, part)], tab.at[pl.ds(n * part, part)], tab_sem.at[n])
                 for n in range(TAB_PARTS)]

    for cp in loads[:2] + tab_loads + loads[2:]:
        cp.start()
    barrier = pltpu.get_barrier_semaphore()

    my_row, my_col = lax.axis_index("rows"), lax.axis_index("cols")
    xs, zs, ys, cs = [around(at, n) for at, n in zip(me, (4, 4, 4, 2))]
    line = [(my_row, y * 2 + c) for y in ys for c in cs]
    plane = [(x * 4 + z, my_col) for x in xs for z in zs]
    for peer in plane[:0:-1] + line[:0:-1]:
        pl.semaphore_signal(barrier, inc=1, device_id=peer, device_id_type=MESH)

    for cp in loads[:2]:
        cp.wait()
    idx = idx_ref[...]
    local_rows = tab.shape[0] // NT
    lane = lax.broadcasted_iota(I32, (16, NDEV), 1)
    table_of = lane // L
    of_table = (lax.broadcasted_iota(I32, (NT, NDEV), 1) // L == lax.broadcasted_iota(I32, (NT, NDEV), 0)).astype(F32)
    limit = dot(len_ref[...].astype(F32), of_table, TN_DIMS).astype(I32)
    live = lane % L < limit
    owner = idx // local_rows
    code = table_of * local_rows + idx % local_rows
    ox, oz, oy, oc = owner // 32, owner // 8 % 4, owner // 2 % 4, owner % 2
    x, z, y, c = me
    slot = (oy - y + 4) % 4 * 32 + (oc - c + 2) % 2 * 16 + (ox - x + 4) % 4 * 4 + (oz - z + 4) % 4
    rel = jnp.where(live, slot, -1)
    bag = lax.broadcasted_iota(I32, (16, NDEV), 0) + 16 * table_of + 1
    sub = lax.broadcasted_iota(I32, (NDEV, NDEV), 0)
    lan = lax.broadcasted_iota(I32, (NDEV, NDEV), 1)
    before = jnp.concatenate([(sub < lan).astype(F32), jnp.ones((NDEV, NDEV), F32)], axis=1).astype(BF16)
    code_hi, code_lo, bag = (code // 256).astype(F32), (code % 256).astype(F32), bag.astype(F32)
    carry = jnp.zeros((NDEV, NDEV), F32)
    ranks = []
    for r in range(16):
        oh = (sub == rel[r:r + 1, :]).astype(F32)
        ohb = oh.astype(BF16)
        counts = dot(ohb, before)
        rank = jnp.sum(oh * (counts[:, :NDEV] + carry), axis=0, keepdims=True).astype(I32)
        carry = carry + counts[:, NDEV:]
        cols = slice(r * NDEV, (r + 1) * NDEV)
        here = sub[:CAP] == rank
        ohs[:, cols] = ohb
        vcode[:CAP, cols] = jnp.where(here, code_hi[r:r + 1], 0.0).astype(BF16)
        vcode[CAP:, cols] = jnp.where(here, code_lo[r:r + 1], 0.0).astype(BF16)
        ranks.append(rank)
    all_oh = ohs[...]
    box = dot(all_oh, vcode[...], NT_DIMS)
    box = box[:, :CAP] * 256.0 + box[:, CAP:]
    outbox[...] = jnp.clip(box.astype(I32), 0, tab.shape[0] - 1).reshape(8, 16, 1, CAP)

    pl.semaphore_wait(barrier, 22)

    def line_copy(n):
        return pltpu.make_async_remote_copy(
            src_ref=outbox.at[n], dst_ref=passing.at[:, n // 2 * 2 + c], send_sem=ids_send.at[0], recv_sem=ids_recv.at[0],
            device_id=line[n], device_id_type=MESH)

    def plane_copy(n):
        return pltpu.make_async_remote_copy(
            src_ref=passing.at[n], dst_ref=ids.at[pl.ds(n * 8, 8)], send_sem=ids_send.at[1], recv_sem=ids_recv.at[n],
            device_id=plane[n], device_id_type=MESH)

    for n in range(1, 8):
        line_copy(n).start()
    passing[:, pl.ds(c, 1)] = outbox[0].reshape(16, 1, 1, CAP)

    first = pltpu.make_async_remote_copy(
        src_ref=outbox.at[pl.ds(1, 7)], dst_ref=outbox.at[pl.ds(1, 7)], send_sem=ids_send.at[0],
        recv_sem=ids_recv.at[0], device_id=line[1], device_id_type=MESH)
    def device(kind, da, db, dy, core, sign):
        dx, dz = da + kind * (db - da), db + kind * (da - db)
        return (lax.rem(x + 4 + sign * dx, 4) * 4 + lax.rem(z + 4 + sign * dz, 4), lax.rem(y + 4 + sign * dy, 4) * 2 + core)

    def line_at(t, n):
        return (0, NEAR[n], t) if n < 3 else (t, FAR, 0)

    def line_order(slot):
        dy, dc, dx, dz = slot // 32, slot // 16 % 2, slot // 4 % 4, slot % 4
        da, db = dx + c * (dz - dx), dz + c * (dx - dz)
        on_y = db == FAR
        n = jnp.where(db >= FAR, FAR + 3 - db, db)
        t, member = jnp.where(on_y, da, dy), jnp.where(on_y, dy, da)
        return (t * 4 + n) * 2 + member // 2, member % 2 * 2 + (c + dc) % 2

    for r in range(16):
        vbag[:, r * NDEV:(r + 1) * NDEV] = jnp.where(sub % CAP == ranks[r], bag[r:r + 1], 0.0).astype(BF16)
    bags = dot(all_oh, vbag[...], NT_DIMS)
    bags = jnp.where(lan // CAP == line_order(sub)[1], bags, 0.0).astype(BF16)
    pick = (line_order(lan[:32])[0] == sub[:32]).astype(F32).astype(BF16)
    mybags[...] = dot(pick, bags).astype(I32).reshape(32, 1, NDEV)

    def bags_copy(src, t, n, peer):
        return pltpu.make_async_remote_copy(
            src_ref=src, dst_ref=linebags.at[pl.ds((t * 4 + n) * 2, 2)], send_sem=bag_send.at[1],
            recv_sem=bag_recv.at[1], device_id=peer, device_id_type=MESH)

    def relay_copy(t):
        return pltpu.make_async_remote_copy(
            src_ref=mybags.at[pl.ds(t * 8, 6)], dst_ref=bagpass.at[pl.ds((t - 1) * 6, 6)], send_sem=bag_send.at[0],
            recv_sem=bag_recv.at[0], device_id=(my_row, ys[t] * 2 + c), device_id_type=MESH)

    for t in range(1, 4):
        relay_copy(t).start()
    for t, n in ((0, 1), (0, 2), (0, 3), (1, 3), (2, 3), (3, 3)):
        bags_copy(mybags.at[pl.ds((t * 4 + n) * 2, 2)], t, n, device(c, *line_at(t, n), c, 1)).start()
    linebags[0:2] = mybags[0:2]
    first.wait_recv()
    for n in range(1, 16):
        plane_copy(n).start()
    own = pltpu.make_async_copy(passing.at[0], ids.at[pl.ds(0, 8)], smem_sem)
    own.start()
    relayed = pltpu.make_async_remote_copy(
        src_ref=bagpass.at[pl.ds(0, 18)], dst_ref=bagpass.at[pl.ds(0, 18)], send_sem=bag_send.at[0],
        recv_sem=bag_recv.at[0], device_id=line[1], device_id_type=MESH)
    relayed.wait_recv()
    for t in range(1, 4):
        linebags[t * 8:t * 8 + 2] = bagpass[(t - 1) * 6:(t - 1) * 6 + 2]
        for n in (1, 2):
            bags_copy(bagpass.at[pl.ds((t - 1) * 6 + n * 2, 2)], t, n, device(c, 0, NEAR[n], 0, c, 1)).start()

    for cp in loads[2:]:
        cp.wait()
    dense = dense_ref[...]
    hidden = lax.dot_general(dense, wd[...], NN_DIMS, precision=lax.Precision.HIGHEST,
                             preferred_element_type=F32) + bias[...]
    for cp in tab_loads:
        cp.wait()


    def block(dst, at, e):
        for j in range(CAP):
            dst[(*at, slice(j, j + 1))] = tab[pl.ds(ids[e, 0, j], 1), :]

    def rows_copy(src, dst, t, peer):
        return pltpu.make_async_remote_copy(
            src_ref=src, dst_ref=dst, send_sem=row_send, recv_sem=row_recv.at[t], device_id=peer, device_id_type=MESH)

    def spot(t, n, m):
        return (m, NEAR[n], t) if n < 3 else (t, FAR, m)

    def stage_at(kind, t, n, m):
        return ((kind * 4 + m) * 4 + n) * 4 + t

    def take(kind, t, n, m):
        da, db, dy = spot(t, n, m)
        block(stage, (stage_at(kind, t, n, m),), ((db * 4 + da) if kind else (da * 4 + db)) * 8 + dy * 2 + kind)

    def here(chunk, kind, t, n):
        at = stage_at(kind, t, n, 0)

        @pl.when(c == kind)
        def _():
            agg[t, n, 0, kind] = stage[at]

        @pl.when(c != kind)
        def _():
            rows_copy(stage.at[at], agg.at[t, n, 0, 1 - kind], chunk, (my_row, y * 2 + kind)).start()

    def push(t):
        lines = [(t, n) for n in range(3)] + [(a, 3) for a in FAR_LINES[t]]
        for m in (1, 2, 3, 0):
            for kind in range(2):
                for a, n in lines:
                    take(kind, a, n, m)
                    if m:
                        away = (m, 0, 0) if n < 3 else (0, 0, m)
                        rows_copy(stage.at[stage_at(kind, a, n, m)], agg.at[a, n, m, c], t,
                                  device(kind, *away, kind, -1)).start()
                    else:
                        here(t, kind, a, n)

    def push_early(ts):
        waited = set()
        for u, v in PLANE_PAIRS:
            for p in sorted({u * 4 + v, v * 4 + u} - waited):
                waited.add(p)
                if p:
                    plane_copy(p).wait_recv()
                else:
                    own.wait()
            for t in ts:
                spots = [(t, NEAR.index(b), m) for m, b in sorted({(u, v), (v, u)}) if b in NEAR]
                if FAR in (u, v) and u + v - FAR in FAR_LINES[t]:
                    spots += [(u + v - FAR, 3, m) for m in range(4)]
                for a, n, m in spots:
                    for kind in range(2):
                        take(kind, a, n, m)
                        if m:
                            away = (m, 0, 0) if n < 3 else (0, 0, m)
                            rows_copy(stage.at[stage_at(kind, a, n, m)], agg.at[a, n, m, c], t,
                                      device(kind, *away, kind, -1)).start()
                        else:
                            here(t, kind, a, n)

    def count(blocks, sem):
        return pltpu.make_async_remote_copy(
            src_ref=stage.at[pl.ds(0, blocks)], dst_ref=stage.at[pl.ds(0, blocks)], send_sem=sem, recv_sem=sem,
            device_id=line[1], device_id_type=MESH)

    all_bags = pltpu.make_async_remote_copy(
        src_ref=mybags.at[pl.ds(0, 24)], dst_ref=linebags.at[pl.ds(0, 24)], send_sem=bag_send.at[1], recv_sem=bag_recv.at[1],
        device_id=line[1], device_id_type=MESH)
    want = lax.broadcasted_iota(I32, (BAGS, NDEV), 0) + 1

    def sum_copy(chunk, t, n):
        return pltpu.make_async_remote_copy(
            src_ref=sums.at[t * 4 + n], dst_ref=parts.at[t * 4 + n], send_sem=sum_send, recv_sem=sum_recv.at[chunk],
            device_id=device(c, *line_at(t, n), c, -1), device_id_type=MESH)

    def sums_of(blocks, t):
        return pltpu.make_async_remote_copy(
            src_ref=sums.at[pl.ds(0, blocks)], dst_ref=parts.at[pl.ds(0, blocks)], send_sem=sum_send,
            recv_sem=sum_recv.at[t], device_id=line[1], device_id_type=MESH)

    def chunk_lines(t):
        return [(a, 3) for a in FAR_LINES[t]] + [(t, n) for n in (2, 1, 0)]

    def pool(chunk):
        count(7 * len(chunk_lines(chunk)), row_recv.at[chunk]).wait_recv()
        for t, n in chunk_lines(chunk):
            at = (t * 4 + n) * 2
            w = jnp.concatenate([(want == linebags[at + h]).astype(F32) for h in range(2)], axis=1).astype(BF16)
            hi, lo = split2(agg[t, n].reshape(8 * CAP, E))
            part = dot(w, hi) + dot(w, lo)
            if t or n:
                sums[t * 4 + n] = part
                sum_copy(chunk, t, n).start()
            else:
                parts[0] = part

    push_early(ORDER[:EARLY])
    for t in ORDER[EARLY:]:
        push(t)
    all_bags.wait_recv()
    for t in ORDER:
        pool(t)

    total = jnp.zeros((BAGS, E), F32)
    for chunk in ORDER:
        lines = chunk_lines(chunk)
        sums_of(len(lines) - (chunk == 0), chunk).wait_recv()
        for t, n in lines:
            total = total + parts[t * 4 + n]

    feats = [dense] + [total[t * 16:(t + 1) * 16] for t in range(NT)]
    for t in range(NT):
        pooled_out[:, t, :] = feats[t + 1]
    k = 0
    for a in range(NT + 1):
        for b in range(a + 1, NT + 1):
            d = jnp.sum(feats[a] * feats[b], axis=-1, keepdims=True)
            hidden = hidden + d * wp[k:k + 1, :]
            k += 1
    hidden_out[...] = jnp.maximum(hidden, 0.0)

    first.wait_send()
    pltpu.make_async_remote_copy(
        src_ref=passing.at[pl.ds(1, 15)], dst_ref=passing.at[pl.ds(1, 15)], send_sem=ids_send.at[1],
        recv_sem=ids_recv.at[1], device_id=plane[1], device_id_type=MESH).wait_send()
    relayed.wait_send()
    all_bags.wait_send()
    count(112, row_send).wait_send()
    pltpu.make_async_remote_copy(
        src_ref=sums.at[pl.ds(1, 15)], dst_ref=parts.at[pl.ds(1, 15)], send_sem=sum_send, recv_sem=sum_recv.at[0],
        device_id=line[1], device_id_type=MESH).wait_send()


def put_out(pooled, hidden, pooled_out, hidden_out, sems):
    copies = [pltpu.make_async_copy(pooled, pooled_out, sems.at[0]), pltpu.make_async_copy(hidden, hidden_out, sems.at[1])]
    for cp in copies:
        cp.start()
    for cp in copies:
        cp.wait()


def shards(bag_index, bag_length, emb_tables, dense_feats, w_dense, w_pair, top_bias):
    rows = NT * emb_tables.shape[1]
    hidden = w_dense.shape[1]
    slots = 16 * NDEV
    vmem, hbm = pl.BlockSpec(memory_space=pltpu.VMEM), pl.BlockSpec(memory_space=pltpu.HBM)
    outs = (jax.ShapeDtypeStruct((16, NT, E), F32), jax.ShapeDtypeStruct((16, hidden), F32))
    found = pl.pallas_call(
        kernel,
        out_shape=outs,
        in_specs=[hbm] * 7,
        out_specs=(vmem, vmem),
        scratch_shapes=[
            pltpu.VMEM((16, NDEV), I32),
            pltpu.VMEM((NT, 16), I32),
            pltpu.VMEM((rows, E), F32),
            pltpu.VMEM((16, E), F32),
            pltpu.VMEM(w_dense.shape, F32),
            pltpu.VMEM(w_pair.shape, F32),
            pltpu.VMEM((1, hidden), F32),
            pltpu.VMEM((NDEV, slots), BF16),
            pltpu.VMEM((2 * CAP, slots), BF16),
            pltpu.VMEM((NDEV, slots), BF16),
            pltpu.VMEM((8, 16, 1, CAP), I32),
            pltpu.VMEM((16, 8, 1, CAP), I32),
            pltpu.SMEM((NDEV, 1, CAP), I32),
            pltpu.VMEM((32, 1, NDEV), I32),
            pltpu.VMEM((18, 1, NDEV), I32),
            pltpu.VMEM((32, 1, NDEV), I32),
            pltpu.VMEM((NDEV, CAP, E), F32),
            pltpu.VMEM((4, 4, 4, 2, CAP, E), F32),
            pltpu.VMEM((16, BAGS, E), F32),
            pltpu.VMEM((16, BAGS, E), F32),
            pltpu.SemaphoreType.DMA((6,)),
            pltpu.SemaphoreType.DMA((TAB_PARTS,)),
            pltpu.SemaphoreType.DMA((2,)),
            pltpu.SemaphoreType.DMA((16,)),
            pltpu.SemaphoreType.DMA,
            pltpu.SemaphoreType.DMA((2,)),
            pltpu.SemaphoreType.DMA((2,)),
            pltpu.SemaphoreType.DMA,
            pltpu.SemaphoreType.DMA((4,)),
            pltpu.SemaphoreType.DMA,
            pltpu.SemaphoreType.DMA((4,)),
        ],
        compiler_params=pltpu.CompilerParams(
            collective_id=0, has_side_effects=True, vmem_limit_bytes=40 * 1024 * 1024),
    )(*[pltpu.with_memory_space_constraint(a, pltpu.HBM) for a in (
        bag_index, bag_length.T, emb_tables.reshape(rows, E), dense_feats, w_dense, w_pair,
        top_bias.reshape(1, hidden))])
    return pl.pallas_call(
        put_out,
        out_shape=outs,
        in_specs=[vmem, vmem],
        out_specs=(hbm, hbm),
        scratch_shapes=[pltpu.SemaphoreType.DMA((2,))],
    )(*[pltpu.with_memory_space_constraint(a, pltpu.VMEM) for a in found])


def solution(mesh):
    samples = P(("rows", "cols"), None)
    in_specs = (samples, samples, P(None, ("rows", "cols"), None), samples, P(), P(), P())
    out_specs = (P(("rows", "cols"), None, None), samples)
    return jax.shard_map(shards, mesh=mesh, in_specs=in_specs, out_specs=out_specs, check_vma=False)
```
